128 devices in a mesh: pi: 8 (over y, x_lo), pj: 16 (over x_hi, z, core).
Axes of the slice: x: 4 (x_hi: 2, x_lo: 2; x = x_hi * 2 + x_lo), y: 4, z: 4, core: 2. Of those that a mesh axis runs over, the one named last changes fastest.
Arguments:
- duo_embedding: bfloat16 [2048, 2048, 128], P('pi', 'pj'), may hold values from -12 to 12
- duo_attention_weights: float32 [128, 8], replicated, may hold values from -16 to 16
- aligned_embedding: bfloat16 [512, 64, 2048], P('pj', None, 'pi'), may hold values from -6 to 6
- aligned_scaling_weights: float32 [64], replicated, may hold values from 0.5 to 1.5
- aligned_shift_vector: float32 [64], replicated, may hold values from -3 to 3
- payload_weights: bfloat16 [64, 256], replicated, may hold values from -0.75 to 0.75
- switch_weights: bfloat16 [64, 256], replicated, may hold values from -0.75 to 0.75
- closing_weights: bfloat16 [256, 64], replicated, may hold values from -1.5 to 1.5
Outputs:
- update: bfloat16 [512, 64, 2048], P('pj', None, 'pi')
The draws below stay inside these ranges and needn't reach their ends.
All inputs are finite; a program needn't handle non-finite values.
Results may differ from the reference program's by a relative error of at most 0.009.
Values may be sent and summed in bfloat16 or wider, within the bound.
A program may use at most 192 MiB of HBM per device.

```python
import math
import jax
import jax.numpy as jnp
from jax import lax

ALIGNED_EMBED = 64
CZ = 128
ATTENDER_TALLY = 8
UNIT_SPAN = 32
POSITION_TALLY = 2048
ALIGNED_SEQS = 512
JOINT_SPAN = 256


def head_directions(key):
    random_dirs = jax.random.normal(jax.random.fold_in(key, 7001), (ATTENDER_TALLY, CZ), jnp.float32)
    random_dirs = random_dirs - jnp.mean(random_dirs, axis=1, keepdims=True)
    return random_dirs / jnp.sqrt(jnp.sum(random_dirs * random_dirs, axis=1, keepdims=True))


def score_weights(key):
    directions = head_directions(key)
    noise = jnp.clip(jax.random.normal(jax.random.fold_in(key, 7002), (CZ, ATTENDER_TALLY), jnp.float32), -6.0, 6.0)
    return 0.18 * noise + 0.35 * directions.T


def draw_duo_attention_weights(key, part):
    return score_weights(key)


def draw_duo_embedding(key, part):
    directions = head_directions(key)
    noise = jnp.clip(jax.random.normal(jax.random.fold_in(key, 7003), (POSITION_TALLY, POSITION_TALLY, CZ), jnp.float32), -6.0, 6.0)
    column_ramp = 2.0 * (2.0 * jnp.arange(POSITION_TALLY, dtype=jnp.float32) / (POSITION_TALLY - 1) - 1.0)
    pair_field = noise + column_ramp[None, :, None] * jnp.sum(directions, axis=0)[None, None, :]
    return pair_field.astype(jnp.bfloat16)


def level_of(key, extent, shards, least, high):
    loudness = 1.0
    for position, blocks in shards:
        heights = jax.random.uniform(jax.random.fold_in(jax.random.fold_in(key, 6), position), (blocks,), jnp.float32, least / len(shards), high / len(shards))
        loudness = loudness * jnp.repeat(jnp.exp(heights), extent[position] // blocks).reshape((-1,) + (1,) * (len(extent) - 1 - position))
    return loudness


def scatter_about(stream_key, extent, width, reach, cuts=(), kind=jnp.bfloat16):
    factor_of = level_of(stream_key, extent, cuts, -0.22, 0.18) if cuts else 1.0
    array = jax.random.normal(stream_key, extent, jnp.float32) * width * factor_of
    return jnp.minimum(jnp.maximum(array, -reach), reach).astype(kind)


def setup_inputs(seed: int = 0) -> dict:
    streams_of = jax.random.split(jax.random.key(seed), 9)
    return {
        "duo_embedding": draw_duo_embedding(jax.random.fold_in(streams_of[8], 71), 0),
        "duo_attention_weights": draw_duo_attention_weights(jax.random.fold_in(streams_of[8], 71), 0),
        "aligned_embedding": scatter_about(streams_of[2], (ALIGNED_SEQS, ALIGNED_EMBED, POSITION_TALLY), 1.0, 6.0, ((0, 16), (2, 8))),
        "aligned_scaling_weights": jnp.clip(1.0 + 0.1 * jax.random.normal(streams_of[3], (ALIGNED_EMBED,), jnp.float32), 0.5, 1.5),
        "aligned_shift_vector": scatter_about(streams_of[4], (ALIGNED_EMBED,), 0.5, 3.0, (), jnp.float32),
        "payload_weights": scatter_about(streams_of[5], (ALIGNED_EMBED, JOINT_SPAN), ALIGNED_EMBED ** -0.5, 0.75),
        "switch_weights": scatter_about(streams_of[6], (ALIGNED_EMBED, JOINT_SPAN), ALIGNED_EMBED ** -0.5, 0.75),
        "closing_weights": scatter_about(streams_of[7], (JOINT_SPAN, ALIGNED_EMBED), (JOINT_SPAN // 16) ** -0.5, 1.5),
    }


EPS = 1e-05

def rescale_embedding(inputs, axis):
    row_mean = lax.optimization_barrier(jnp.mean(inputs, axis=axis, keepdims=True))
    centred = inputs - row_mean
    variance = lax.optimization_barrier(jnp.mean(centred * centred, axis=axis, keepdims=True))
    return centred * lax.rsqrt(variance + EPS)

def reference(duo_embedding, duo_attention_weights, aligned_embedding, aligned_scaling_weights, aligned_shift_vector, payload_weights, switch_weights, closing_weights):
    aligned_fullbit_copy = aligned_embedding.astype(jnp.float32)
    rescaled_aligned = (rescale_embedding(aligned_fullbit_copy, 1) * aligned_scaling_weights[None, :, None] + aligned_shift_vector[None, :, None]).astype(jnp.bfloat16)
    normed_float = rescaled_aligned.astype(jnp.float32)
    payloads = jnp.einsum('scn,ce->sen', normed_float, payload_weights.astype(jnp.float32)).astype(jnp.bfloat16)
    switch_share = jax.nn.sigmoid(jnp.einsum('scn,ce->sen', normed_float, switch_weights.astype(jnp.float32)))
    payload_each_attender = payloads.astype(jnp.float32).reshape(ALIGNED_SEQS, ATTENDER_TALLY, UNIT_SPAN, POSITION_TALLY)
    tile_entries = math.gcd(POSITION_TALLY, 256)
    block_count = POSITION_TALLY // tile_entries

    def one_block(block_index):
        start_position = (block_index * tile_entries).astype(jnp.int32)
        pair_tile = lax.dynamic_slice_in_dim(duo_embedding, start_position, tile_entries, 0).astype(jnp.float32)
        pair_normed = rescale_embedding(pair_tile, 2)
        scores = jnp.einsum('ijc,ch->hij', pair_normed, duo_attention_weights, precision=lax.Precision.HIGHEST)
        row_peak = lax.optimization_barrier(jnp.max(scores, axis=2, keepdims=True))
        exp_scores = jnp.exp(scores - row_peak).astype(jnp.bfloat16)
        exp_float = exp_scores.astype(jnp.float32)
        row_total = lax.optimization_barrier(jnp.sum(exp_float, axis=2))
        numerator = jnp.einsum('hij,shcj->shci', exp_float, payload_each_attender)
        switch_tile = lax.dynamic_slice_in_dim(switch_share, start_position, tile_entries, 2).reshape(ALIGNED_SEQS, ATTENDER_TALLY, UNIT_SPAN, tile_entries)
        averaged_result = (switch_tile * (numerator / row_total[None, :, None, :])).astype(jnp.bfloat16)
        averaged_result = averaged_result.reshape(ALIGNED_SEQS, ATTENDER_TALLY * UNIT_SPAN, tile_entries).astype(jnp.float32)
        return jnp.einsum('ser,ec->scr', averaged_result, closing_weights.astype(jnp.float32)).astype(jnp.bfloat16)
    result_tiles = lax.map(one_block, jnp.arange(block_count, dtype=jnp.int32))
    return jnp.transpose(result_tiles, (1, 2, 0, 3)).reshape(ALIGNED_SEQS, ALIGNED_EMBED, POSITION_TALLY)
```

```python
import functools

import jax
import jax.numpy as jnp
from jax import lax
from jax.experimental import pallas as pl
from jax.experimental.pallas import tpu as pltpu
from jax.sharding import PartitionSpec as P

EPS = 1e-05
F32 = jnp.float32
BF16 = jnp.bfloat16
MESH = pl.DeviceIdType.MESH
NT = (((1,), (1,)), ((), ()))

HEADS = 8
SPAN = 32
ROWS = 32
CH = 64
TOK = 256
X_ROWS = 24
NPIECES = 8


def kernel(
    duo_hbm, wt_ref, msa_ref, gain_ref, shift_ref, pw_ref, sw_ref, cw_ref,
    out_ref,
    nbuf, ebuf, duo, sc, st, mx, acc, gate, vbuf, tot, pwt, swt, cwt, gcol,
    duo_sem, n_send, n_recv, e_send, e_recv, m_send, m_recv,
):
    pi = lax.axis_index("pi")
    pj = lax.axis_index("pj")
    y, xl = lax.div(pi, 2), lax.rem(pi, 2)
    xh, zc = lax.div(pj, 8), lax.rem(pj, 8)
    z, core = lax.div(zc, 2), lax.rem(zc, 2)

    def pi_of(yy, ll):
        return yy * 2 + ll

    def pj_of(hh, zz, cc):
        return hh * 8 + zz * 2 + cc

    yp, ym, yo = lax.rem(y + 1, 4), lax.rem(y + 3, 4), lax.rem(y + 2, 4)
    zp, zm, zo = lax.rem(z + 1, 4), lax.rem(z + 3, 4), lax.rem(z + 2, 4)
    ol, oh = 1 - xl, 1 - xh

    step = 256 // NPIECES

    def duo_copy(k):
        rows = pl.ds(k * step, step)
        return pltpu.make_async_copy(duo_hbm.at[rows], duo.at[rows], duo_sem.at[k])

    for k in range(NPIECES):
        duo_copy(k).start()

    barrier = pltpu.get_barrier_semaphore()
    for d in range(1, 16):
        pl.semaphore_signal(
            barrier, inc=1, device_id={"pi": pi, "pj": lax.rem(pj + d, 16)}, device_id_type=MESH
        )
    for other in (pi_of(yp, xl), pi_of(ym, xl), pi_of(y, ol)):
        pl.semaphore_signal(
            barrier, inc=1, device_id={"pi": other, "pj": pj}, device_id_type=MESH
        )

    def column(ref):
        row = jnp.broadcast_to(ref[...], (CH, CH))
        r = lax.broadcasted_iota(jnp.int32, (CH, CH), 0)
        c = lax.broadcasted_iota(jnp.int32, (CH, CH), 1)
        col = jnp.sum(jnp.where(r == c, row, 0.0), axis=1, keepdims=True)
        return jnp.broadcast_to(col, (CH, TOK))

    gcol[0] = column(gain_ref)
    gcol[1] = column(shift_ref)

    def norm_row(s, _):
        v = msa_ref[s].astype(F32)
        mean = jnp.mean(v, axis=0, keepdims=True)
        v = v - mean
        var = jnp.mean(v * v, axis=0, keepdims=True)
        v = v * lax.rsqrt(var + EPS)
        nbuf[pi, s] = (v * gcol[0] + gcol[1]).astype(BF16)
        return 0

    lax.fori_loop(0, ROWS, norm_row, 0)
    pl.semaphore_wait(barrier, 18)

    xa, xb = X_ROWS // 2, X_ROWS
    ya, yb = X_ROWS + (ROWS - X_ROWS) // 2, ROWS

    def n_copy(k, block, lo, hi, to_y, to_l):
        view = nbuf.at[block, pl.ds(lo, hi - lo)]
        return pltpu.make_async_remote_copy(
            src_ref=view, dst_ref=view, send_sem=n_send.at[k], recv_sem=n_recv.at[k],
            device_id={"pi": pi_of(to_y, to_l), "pj": pj}, device_id_type=MESH,
        )

    own, part = pi, pi_of(y, ol)
    b_m, b_p, b_o = pi_of(ym, xl), pi_of(yp, xl), pi_of(yo, xl)
    q_m, q_p = pi_of(ym, ol), pi_of(yp, ol)
    n = [
        n_copy(0, own, 0, xb, y, ol),
        n_copy(1, own, xb, yb, y, ol),
        n_copy(2, own, xb, yb, yp, xl),
        n_copy(3, own, 0, xb, yp, xl),
        n_copy(4, own, xb, yb, ym, xl),
        n_copy(5, own, 0, xb, ym, xl),
        n_copy(6, b_m, xb, ya, yp, xl),
        n_copy(7, b_p, ya, yb, ym, xl),
        n_copy(8, b_m, xb, yb, y, ol),
        n_copy(9, b_p, xb, yb, y, ol),
        n_copy(10, b_o, xb, ya, y, ol),
        n_copy(11, b_o, ya, yb, y, ol),
        n_copy(12, part, 0, xb, yp, xl),
        n_copy(13, part, 0, xb, ym, xl),
        n_copy(14, b_m, 0, xa, yp, xl),
        n_copy(15, b_p, xa, xb, ym, xl),
        n_copy(16, q_m, 0, xa, yp, xl),
        n_copy(17, q_p, xa, xb, ym, xl),
    ]
    for k in (2, 4, 0, 3, 5):
        n[k].start()

    pwt[...] = pw_ref[...].astype(F32).T.astype(BF16)
    swt[...] = sw_ref[...].astype(F32).T.astype(BF16)
    cwt[...] = cw_ref[...].astype(F32).T.astype(BF16)

    w = wt_ref[...]
    w = w - jnp.mean(w, axis=1, keepdims=True)
    w_sum = jnp.sum(w, axis=1, keepdims=True)
    w_hi = w.astype(BF16)
    w_rest = w - w_hi.astype(F32)
    w_mid = w_rest.astype(BF16)
    w_lo = (w_rest - w_mid.astype(F32)).astype(BF16)
    ones8 = jnp.ones((8, 128), F32)
    stack = jnp.concatenate(
        [w_hi.astype(F32), w_mid.astype(F32), w_lo.astype(F32), ones8], axis=0
    ).astype(BF16)
    ones = jnp.ones((16, 128), BF16)
    group = 16

    def score_group(g, _):
        i0 = g * group
        x = duo[pl.ds(i0, group)].reshape(group * 128, 128)
        xf = x.astype(F32)
        sq = xf * xf
        sq_hi = sq.astype(BF16)
        sq_lo = (sq - sq_hi.astype(F32)).astype(BF16)
        r = lax.dot_general(stack, x, NT, preferred_element_type=F32)
        t_hi = lax.dot_general(ones, sq_hi, NT, preferred_element_type=F32)[0:8]
        t_lo = lax.dot_general(ones, sq_lo, NT, preferred_element_type=F32)[0:8]
        mean = r[24:32] * (1.0 / 128)
        m_hi = mean.astype(BF16).astype(F32)
        m_lo = mean - m_hi
        var = t_hi * (1.0 / 128) - m_hi * m_hi
        var = var - 2.0 * m_hi * m_lo
        var = (var - m_lo * m_lo) + t_lo * (1.0 / 128)
        var = jnp.maximum(var, 0.0)
        dots = (r[16:24] + r[8:16]) + r[0:8]
        s = (dots - mean * w_sum) * lax.rsqrt(var + EPS)
        for a in range(group):
            rows = pl.ds(pl.multiple_of((i0 + a) * 8, 8), 8)
            sc[rows, :] = s[:, a * 128:(a + 1) * 128]
        return 0

    per = step // group

    def score_piece(k, _):
        duo_copy(k).wait()
        lax.fori_loop(k * per, (k + 1) * per, score_group, 0)
        return 0

    lax.fori_loop(0, NPIECES, score_piece, 0)

    for h in range(HEADS):
        t = sc[pl.ds(h, 256, stride=8), :].T
        st[h] = t
        mx[pj, pl.ds(h, 1), :] = jnp.max(t, axis=0, keepdims=True)

    def m_copy(d):
        return pltpu.make_async_remote_copy(
            src_ref=mx.at[pj], dst_ref=mx.at[pj], send_sem=m_send.at[d - 1],
            recv_sem=m_recv.at[d - 1],
            device_id={"pi": pi, "pj": lax.rem(pj + d, 16)}, device_id_type=MESH,
        )

    for d in range(1, 16):
        m_copy(d).start()

    n[2].wait_recv()
    n[6].start()
    n[4].wait_recv()
    n[7].start()

    def gate_row(s, _):
        g = jnp.dot(swt[...], nbuf[pi, s], preferred_element_type=F32)
        gate[s] = jax.nn.sigmoid(g)
        return 0

    lax.fori_loop(0, ROWS, gate_row, 0)

    for d in range(1, 16):
        m_copy(d).wait_recv()
    peak = mx[0]
    for d in range(1, 16):
        peak = jnp.maximum(peak, mx[d])
    mx_peak = peak

    block = xh * 4 + z
    half = pl.ds(pl.multiple_of(core * 128, 128), 128)
    for h in range(HEADS):
        ebuf[block, h, half, :] = jnp.exp(st[h] - mx_peak[h:h + 1]).astype(BF16)

    def e_copy(k, hh, zz, h0, h1, to_h, to_z, to_c):
        view = ebuf.at[hh * 4 + zz, pl.ds(h0, h1 - h0), half]
        return pltpu.make_async_remote_copy(
            src_ref=view, dst_ref=view, send_sem=e_send.at[k], recv_sem=e_recv.at[k],
            device_id={"pi": pi, "pj": pj_of(to_h, to_z, to_c)}, device_id_type=MESH,
        )

    oc = 1 - core
    e = [
        e_copy(0, xh, z, 0, 8, xh, z, oc),
        e_copy(1, xh, z, 0, 8, oh, z, core),
        e_copy(2, xh, z, 0, 8, xh, zp, core),
        e_copy(3, xh, z, 0, 8, xh, zm, core),
        e_copy(4, oh, z, 0, 8, xh, zp, core),
        e_copy(5, oh, z, 0, 8, xh, zm, core),
        e_copy(6, oh, z, 0, 8, xh, z, oc),
        e_copy(7, xh, zm, 0, 4, xh, zp, core),
        e_copy(8, xh, zm, 0, 8, xh, z, oc),
        e_copy(9, xh, zp, 4, 8, xh, zm, core),
        e_copy(10, xh, zp, 0, 8, xh, z, oc),
        e_copy(11, xh, zo, 0, 4, xh, z, oc),
        e_copy(12, xh, zo, 4, 8, xh, z, oc),
        e_copy(13, oh, zm, 0, 4, xh, zp, core),
        e_copy(14, oh, zm, 0, 8, xh, z, oc),
        e_copy(15, oh, zp, 4, 8, xh, zm, core),
        e_copy(16, oh, zp, 0, 8, xh, z, oc),
        e_copy(17, oh, zo, 0, 4, xh, z, oc),
        e_copy(18, oh, zo, 4, 8, xh, z, oc),
    ]
    for k in (1, 2, 3, 0):
        e[k].start()
    for k in (1, 8, 9):
        n[k].start()

    acc[...] = jnp.zeros_like(acc)
    tot[...] = jnp.zeros_like(tot)

    n[0].wait_recv()
    n[12].start()
    n[13].start()
    n[3].wait_recv()
    n[14].start()
    n[5].wait_recv()
    n[15].start()
    n[6].wait_recv()
    n[10].start()
    n[7].wait_recv()
    n[11].start()
    e[2].wait_recv()
    e[7].start()
    e[8].start()
    e[3].wait_recv()
    e[9].start()
    e[10].start()
    e[1].wait_recv()
    for k in (4, 5, 6):
        e[k].start()
    e[7].wait_recv()
    e[11].start()
    e[9].wait_recv()
    e[12].start()
    n[12].wait_recv()
    n[16].start()
    n[13].wait_recv()
    n[17].start()
    e[4].wait_recv()
    e[13].start()
    e[14].start()
    e[5].wait_recv()
    e[15].start()
    e[16].start()
    e[13].wait_recv()
    e[17].start()
    e[15].wait_recv()
    e[18].start()
    for k in (0, 8, 10, 11, 12, 6, 14, 16, 17, 18):
        e[k].wait_recv()

    ones_t = jnp.ones((16, TOK), BF16)

    def value_row(p, s, _):
        v = jnp.dot(pwt[...], nbuf[p, s], preferred_element_type=F32)
        vbuf[s] = v.astype(BF16)
        return 0

    def head_step(p, h, _):
        rows = pl.ds(pl.multiple_of(h * SPAN, SPAN), SPAN)
        weights = ebuf[p, h]
        v = vbuf[:, rows, :].reshape(ROWS * SPAN, TOK)
        part_sum = jnp.dot(v, weights, preferred_element_type=F32)
        acc[:, rows, :] += part_sum.reshape(ROWS, SPAN, TOK)
        tot[h] += jnp.dot(ones_t, weights, preferred_element_type=F32)[0:8]
        return 0

    def one_block(p):
        lax.fori_loop(0, ROWS, functools.partial(value_row, p), 0)
        lax.fori_loop(0, HEADS, functools.partial(head_step, p), 0)

    one_block(own)
    one_block(b_m)
    one_block(b_p)
    n[1].wait_recv()
    one_block(part)
    n[8].wait_recv()
    one_block(q_m)
    n[9].wait_recv()
    one_block(q_p)
    n[14].wait_recv()
    n[15].wait_recv()
    one_block(b_o)
    for k in (10, 11, 16, 17):
        n[k].wait_recv()
    one_block(pi_of(yo, ol))

    for h in range(HEADS):
        tot[h] = 1.0 / tot[h]

    def out_row(s, _):
        pieces = []
        for h in range(HEADS):
            rows = slice(h * SPAN, (h + 1) * SPAN)
            share = tot[h, 0:1, :]
            pieces.append((gate[s, rows, :] * (acc[s, rows, :] * share)).astype(BF16))
        mixed = jnp.concatenate(pieces, axis=0)
        out_ref[s] = jnp.dot(cwt[...], mixed, preferred_element_type=F32).astype(BF16)
        return 0

    lax.fori_loop(0, ROWS, out_row, 0)

    for c in n + e:
        c.wait_send()
    for d in range(1, 16):
        m_copy(d).wait_send()


def body(duo, w, msa, gain, shift, pw, sw, cw):
    vm = pl.BlockSpec(memory_space=pltpu.VMEM)
    return pl.pallas_call(
        kernel,
        out_shape=jax.ShapeDtypeStruct((ROWS, CH, TOK), BF16),
        in_specs=[pl.BlockSpec(memory_space=pl.ANY)] + [vm] * 7,
        out_specs=vm,
        scratch_shapes=[
            pltpu.VMEM((8, ROWS, CH, TOK), BF16),
            pltpu.VMEM((8, HEADS, TOK, TOK), BF16),
            pltpu.VMEM((256, 128, 128), BF16),
            pltpu.VMEM((256 * HEADS, 128), F32),
            pltpu.VMEM((HEADS, 128, TOK), F32),
            pltpu.VMEM((16, HEADS, TOK), F32),
            pltpu.VMEM((ROWS, 256, TOK), F32),
            pltpu.VMEM((ROWS, 256, TOK), F32),
            pltpu.VMEM((ROWS, 256, TOK), BF16),
            pltpu.VMEM((HEADS, 8, TOK), F32),
            pltpu.VMEM((256, CH), BF16),
            pltpu.VMEM((256, CH), BF16),
            pltpu.VMEM((CH, 256), BF16),
            pltpu.VMEM((2, CH, TOK), F32),
            pltpu.SemaphoreType.DMA((NPIECES,)),
            pltpu.SemaphoreType.DMA((18,)),
            pltpu.SemaphoreType.DMA((18,)),
            pltpu.SemaphoreType.DMA((19,)),
            pltpu.SemaphoreType.DMA((19,)),
            pltpu.SemaphoreType.DMA((15,)),
            pltpu.SemaphoreType.DMA((15,)),
        ],
        compiler_params=pltpu.CompilerParams(
            collective_id=0, has_side_effects=True, vmem_limit_bytes=66_000_000
        ),
        name="pair_average",
    )(duo, w.T, msa, gain.reshape(1, CH), shift.reshape(1, CH), pw, sw, cw)


def solution(mesh):
    placed = (P("pi", "pj", None), P(), P("pj", None, "pi"), P(), P(), P(), P(), P())
    return jax.shard_map(
        body, mesh=mesh, in_specs=placed, out_specs=P("pj", None, "pi"), check_vma=False
    )
```

```python
import functools

import jax
import jax.numpy as jnp
from jax import lax
from jax.experimental import pallas as pl
from jax.experimental.pallas import tpu as pltpu
from jax.sharding import PartitionSpec as P

EPS = 1e-05
F32 = jnp.float32
BF16 = jnp.bfloat16
MESH = pl.DeviceIdType.MESH
NT = (((1,), (1,)), ((), ()))

HEADS = 8
SPAN = 32
ROWS = 32
CH = 64
TOK = 256
X_ROWS = 22
NPIECES = 8


def kernel(
    duo_hbm, wt_ref, msa_ref, gain_ref, shift_ref, pw_ref, sw_ref, cw_ref,
    out_ref,
    nbuf, ebuf, sc, mx, acc, gate, vbuf, tot, pwt, swt, gcol,
    duo_sem, n_send, n_recv, e_send, e_recv, m_send, m_recv,
):
    pi = lax.axis_index("pi")
    pj = lax.axis_index("pj")
    y, xl = lax.div(pi, 2), lax.rem(pi, 2)
    xh, zc = lax.div(pj, 8), lax.rem(pj, 8)
    z, core = lax.div(zc, 2), lax.rem(zc, 2)

    def pi_of(yy, ll):
        return yy * 2 + ll

    def pj_of(hh, zz, cc):
        return hh * 8 + zz * 2 + cc

    yp, ym, yo = lax.rem(y + 1, 4), lax.rem(y + 3, 4), lax.rem(y + 2, 4)
    zp, zm, zo = lax.rem(z + 1, 4), lax.rem(z + 3, 4), lax.rem(z + 2, 4)
    ol, oh = 1 - xl, 1 - xh

    step = 128 // NPIECES

    def duo_copy(k):
        rows = pl.ds(k * step, step)
        there = pl.ds(256 + k * step, step)
        return pltpu.make_async_copy(duo_hbm.at[rows], vbuf.at[there], duo_sem.at[k])

    for k in range(NPIECES):
        duo_copy(k).start()

    barrier = pltpu.get_barrier_semaphore()
    for d in range(1, 16):
        pl.semaphore_signal(
            barrier, inc=1, device_id={"pi": pi, "pj": lax.rem(pj + d, 16)}, device_id_type=MESH
        )
    for other in (pi_of(yp, xl), pi_of(ym, xl), pi_of(y, ol)):
        pl.semaphore_signal(
            barrier, inc=1, device_id={"pi": other, "pj": pj}, device_id_type=MESH
        )

    def column(ref):
        row = jnp.broadcast_to(ref[...], (CH, CH))
        r = lax.broadcasted_iota(jnp.int32, (CH, CH), 0)
        c = lax.broadcasted_iota(jnp.int32, (CH, CH), 1)
        col = jnp.sum(jnp.where(r == c, row, 0.0), axis=1, keepdims=True)
        return jnp.broadcast_to(col, (CH, TOK))

    gcol[0] = column(gain_ref)
    gcol[1] = column(shift_ref)

    def norm_rows(g, _):
        for a in range(4):
            s = g * 4 + a
            v = msa_ref[s].astype(F32)
            mean = jnp.mean(v, axis=0, keepdims=True)
            v = v - mean
            var = jnp.mean(v * v, axis=0, keepdims=True)
            v = v * lax.rsqrt(var + EPS)
            nbuf[pi, s] = (v * gcol[0] + gcol[1]).astype(BF16)
        return 0

    lax.fori_loop(0, ROWS // 4, norm_rows, 0)
    pl.semaphore_wait(barrier, 18)

    xa, xb = X_ROWS // 2, X_ROWS
    ya, yb = X_ROWS + (ROWS - X_ROWS) // 2, ROWS

    def n_copy(k, block, lo, hi, to_y, to_l):
        view = nbuf.at[block, pl.ds(lo, hi - lo)]
        return pltpu.make_async_remote_copy(
            src_ref=view, dst_ref=view, send_sem=n_send.at[k], recv_sem=n_recv.at[k],
            device_id={"pi": pi_of(to_y, to_l), "pj": pj}, device_id_type=MESH,
        )

    own, part = pi, pi_of(y, ol)
    b_m, b_p, b_o = pi_of(ym, xl), pi_of(yp, xl), pi_of(yo, xl)
    q_m, q_p = pi_of(ym, ol), pi_of(yp, ol)
    n = [
        n_copy(0, own, 0, xb, y, ol),
        n_copy(1, own, xb, yb, y, ol),
        n_copy(2, own, xb, yb, yp, xl),
        n_copy(3, own, 0, xb, yp, xl),
        n_copy(4, own, xb, yb, ym, xl),
        n_copy(5, own, 0, xb, ym, xl),
        n_copy(6, b_m, xb, ya, yp, xl),
        n_copy(7, b_p, ya, yb, ym, xl),
        n_copy(8, b_m, xb, yb, y, ol),
        n_copy(9, b_p, xb, yb, y, ol),
        n_copy(10, b_o, xb, ya, y, ol),
        n_copy(11, b_o, ya, yb, y, ol),
        n_copy(12, part, 0, xb, yp, xl),
        n_copy(13, part, 0, xb, ym, xl),
        n_copy(14, b_m, 0, xa, yp, xl),
        n_copy(15, b_p, xa, xb, ym, xl),
        n_copy(16, q_m, 0, xa, yp, xl),
        n_copy(17, q_p, xa, xb, ym, xl),
    ]
    for k in (2, 4, 0, 3, 5):
        n[k].start()

    pwt[...] = pw_ref[...].astype(F32).T.astype(BF16)
    swt[...] = sw_ref[...].astype(F32).T.astype(BF16)

    w = wt_ref[...]
    w = w - jnp.mean(w, axis=1, keepdims=True)
    w_sum = jnp.sum(w, axis=1, keepdims=True)
    w_hi = w.astype(BF16)
    w_rest = w - w_hi.astype(F32)
    w_mid = w_rest.astype(BF16)
    w_lo = (w_rest - w_mid.astype(F32)).astype(BF16)
    ones8 = jnp.ones((8, 128), F32)
    stack = jnp.concatenate(
        [w_hi.astype(F32), w_mid.astype(F32), w_lo.astype(F32), ones8], axis=0
    ).astype(BF16)
    ones = jnp.ones((16, 128), BF16)
    group = 16

    def score_group(g, _):
        x = vbuf[pl.ds(256 + g * (group // 2), group // 2)].reshape(group * 128, 128)
        xf = x.astype(F32)
        sq = xf * xf
        sq_hi = sq.astype(BF16)
        sq_lo = (sq - sq_hi.astype(F32)).astype(BF16)
        r = lax.dot_general(stack, x, NT, preferred_element_type=F32)
        t_hi = lax.dot_general(ones, sq_hi, NT, preferred_element_type=F32)[0:8]
        t_lo = lax.dot_general(ones, sq_lo, NT, preferred_element_type=F32)[0:8]
        mean = r[24:32] * (1.0 / 128)
        m_hi = mean.astype(BF16).astype(F32)
        m_lo = mean - m_hi
        var = t_hi * (1.0 / 128) - m_hi * m_hi
        var = var - 2.0 * m_hi * m_lo
        var = (var - m_lo * m_lo) + t_lo * (1.0 / 128)
        var = jnp.maximum(var, 0.0)
        dots = (r[16:24] + r[8:16]) + r[0:8]
        s = (dots - mean * w_sum) * lax.rsqrt(var + EPS)
        for a in range(group):
            rows = pl.ds(pl.multiple_of((g * group + a) * 8, 8), 8)
            sc[rows, :] = s[:, a * 128:(a + 1) * 128]
        return 0

    per = 2 * step // group

    def score_piece(k, _):
        duo_copy(k).wait()
        lax.fori_loop(k * per, (k + 1) * per, score_group, 0)
        return 0

    def m_copy(r, d):
        view = mx.at[r, pj]
        return pltpu.make_async_remote_copy(
            src_ref=view, dst_ref=view, send_sem=m_send.at[r, d - 1],
            recv_sem=m_recv.at[r, d - 1],
            device_id={"pi": pi, "pj": lax.rem(pj + d, 16)}, device_id_type=MESH,
        )

    def scores_of(r):
        lax.fori_loop(r * NPIECES // 2, (r + 1) * NPIECES // 2, score_piece, 0)
        for h in range(HEADS):
            t = sc[pl.ds(r * 1024 + h, 128, stride=8), :].T
            acc[8 + h, 0:128, r * 128:(r + 1) * 128] = t
            mx[r, pj, pl.ds(h, 1), :] = jnp.max(t, axis=0, keepdims=True)
        for d in range(1, 16):
            m_copy(r, d).start()

    def columns(zz, cc):
        return pl.ds(pl.multiple_of(lax.rem(zz, 2) * 256 + cc * 128, 128), 128)

    def pair_of(hh, zz):
        return hh * 2 + lax.div(zz, 2)

    def exps_of(r):
        for d in range(1, 16):
            m_copy(r, d).wait_recv()
        peak = mx[r, 0]
        for d in range(1, 16):
            peak = jnp.maximum(peak, mx[r, d])
        lanes = slice(r * 128, (r + 1) * 128)
        for h in range(HEADS):
            t = jnp.exp(acc[8 + h, 0:128, lanes] - peak[h:h + 1])
            ebuf[pair_of(xh, z), h, columns(z, core), lanes] = t.astype(BF16)

    def e_copy(r, k, hh, zz, h0, h1, to_h, to_z, to_c):
        view = ebuf.at[
            pair_of(hh, zz), pl.ds(h0, h1 - h0), columns(zz, core), pl.ds(r * 128, 128)
        ]
        return pltpu.make_async_remote_copy(
            src_ref=view, dst_ref=view, send_sem=e_send.at[r, k], recv_sem=e_recv.at[r, k],
            device_id={"pi": pi, "pj": pj_of(to_h, to_z, to_c)}, device_id_type=MESH,
        )

    oc = 1 - core
    e = [
        [
            e_copy(r, 0, xh, z, 0, 8, xh, z, oc),
            e_copy(r, 1, xh, z, 0, 8, oh, z, core),
            e_copy(r, 2, xh, z, 0, 8, xh, zp, core),
            e_copy(r, 3, xh, z, 0, 8, xh, zm, core),
            e_copy(r, 4, oh, z, 0, 8, xh, zp, core),
            e_copy(r, 5, oh, z, 0, 8, xh, zm, core),
            e_copy(r, 6, oh, z, 0, 8, xh, z, oc),
            e_copy(r, 7, xh, zm, 0, 4, xh, zp, core),
            e_copy(r, 8, xh, zm, 0, 8, xh, z, oc),
            e_copy(r, 9, xh, zp, 4, 8, xh, zm, core),
            e_copy(r, 10, xh, zp, 0, 8, xh, z, oc),
            e_copy(r, 11, xh, zo, 0, 4, xh, z, oc),
            e_copy(r, 12, xh, zo, 4, 8, xh, z, oc),
            e_copy(r, 13, oh, zm, 0, 4, xh, zp, core),
            e_copy(r, 14, oh, zm, 0, 8, xh, z, oc),
            e_copy(r, 15, oh, zp, 4, 8, xh, zm, core),
            e_copy(r, 16, oh, zp, 0, 8, xh, z, oc),
            e_copy(r, 17, oh, zo, 0, 4, xh, z, oc),
            e_copy(r, 18, oh, zo, 4, 8, xh, z, oc),
        ]
        for r in range(2)
    ]

    scores_of(0)
    scores_of(1)
    n[2].wait_recv()
    n[6].start()
    n[4].wait_recv()
    n[7].start()
    for r in range(2):
        exps_of(r)
        for k in (2, 3, 1, 0):
            e[r][k].start()
    for k in (1, 8, 9):
        n[k].start()

    acc[...] = jnp.zeros_like(acc)
    tot[...] = jnp.zeros_like(tot)

    def gate_rows(g, _):
        for a in range(4):
            s = g * 4 + a
            t = jnp.dot(swt[...], nbuf[pi, s], preferred_element_type=F32)
            gate[s] = jax.nn.sigmoid(t)
        return 0

    ones_t = jnp.ones((16, 2 * TOK), BF16)

    def value_rows(p, slot, c, g, _):
        for a in range(8):
            s = g * 8 + a
            v = jnp.dot(pwt[...], nbuf[p, s], preferred_element_type=F32).astype(BF16)
            vbuf[slot * 128 + s * 4 + c * 2] = v[:, 0:128]
            vbuf[slot * 128 + s * 4 + c * 2 + 1] = v[:, 128:256]
        return 0

    def head_step(yy, slot, g, _):
        v4 = vbuf.at[pl.ds(slot * 128, 128)]
        for a in range(2):
            h = g * 2 + a
            rows = pl.ds(pl.multiple_of(h * SPAN, SPAN), SPAN)
            weights = ebuf[yy, h]
            v = v4[:, rows, :].reshape(ROWS, 4, SPAN, 128)
            v = jnp.concatenate(
                [v[:, t].reshape(ROWS * SPAN, 128) for t in range(4)], axis=1
            )
            part_sum = jnp.dot(v, weights, preferred_element_type=F32)
            acc[:, rows, :] += part_sum.reshape(ROWS, SPAN, TOK)
            tot[h] += jnp.dot(ones_t, weights, preferred_element_type=F32)[0:8]
        return 0

    def values_of(p, slot, c):
        lax.fori_loop(0, ROWS // 8, functools.partial(value_rows, p, slot, c), 0)

    def product_of(yy, slot):
        lax.fori_loop(0, HEADS // 2, functools.partial(head_step, yy, slot), 0)

    lax.fori_loop(0, ROWS // 4, gate_rows, 0)
    values_of(own, 0, xl)

    def hop(k, *then):
        for r in range(2):
            e[r][k].wait_recv()
            for t in then:
                e[r][t].start()

    n[0].wait_recv()
    n[12].start()
    n[13].start()
    hop(2, 7, 8)
    hop(3, 9, 10)
    n[3].wait_recv()
    n[14].start()
    n[5].wait_recv()
    n[15].start()
    n[6].wait_recv()
    n[10].start()
    n[7].wait_recv()
    n[11].start()
    hop(1, 4, 5, 6)
    values_of(b_m, 1, xl)
    hop(7, 11)
    hop(9, 12)
    values_of(b_p, 2, xl)
    n[1].wait_recv()
    values_of(part, 0, ol)
    hop(4, 13, 14)
    hop(5, 15, 16)
    n[12].wait_recv()
    n[16].start()
    n[13].wait_recv()
    n[17].start()
    n[8].wait_recv()
    values_of(q_m, 1, ol)
    n[9].wait_recv()
    values_of(q_p, 2, ol)
    hop(13, 17)
    hop(15, 18)
    for k in (0, 8, 10, 11, 12, 6, 14, 16, 17, 18):
        hop(k)
    product_of(y, 0)
    product_of(ym, 1)
    n[14].wait_recv()
    n[15].wait_recv()
    values_of(b_o, 0, xl)
    product_of(yp, 2)
    for k in (10, 11, 16, 17):
        n[k].wait_recv()
    values_of(pi_of(yo, ol), 0, ol)
    product_of(yo, 0)

    for h in range(HEADS):
        tot[h] = 1.0 / tot[h]

    def out_rows(g, _):
        for a in range(4):
            s = g * 4 + a
            pieces = []
            for h in range(HEADS):
                rows = slice(h * SPAN, (h + 1) * SPAN)
                share = tot[h, 0:1, :]
                pieces.append((gate[s, rows, :] * (acc[s, rows, :] * share)).astype(BF16))
            mixed = jnp.concatenate(pieces, axis=0)
            out_ref[s] = jnp.dot(cw_ref[...], mixed, preferred_element_type=F32).astype(BF16)
        return 0

    lax.fori_loop(0, ROWS // 4, out_rows, 0)

    for c in n + e[0] + e[1]:
        c.wait_send()
    for r in range(2):
        for d in range(1, 16):
            m_copy(r, d).wait_send()


def body(duo, w, msa, gain, shift, pw, sw, cw):
    vm = pl.BlockSpec(memory_space=pltpu.VMEM)
    return pl.pallas_call(
        kernel,
        out_shape=jax.ShapeDtypeStruct((ROWS, CH, TOK), BF16),
        in_specs=[pl.BlockSpec(memory_space=pl.ANY)] + [vm] * 7,
        out_specs=vm,
        scratch_shapes=[
            pltpu.VMEM((8, ROWS, CH, TOK), BF16),
            pltpu.VMEM((4, HEADS, 2 * TOK, TOK), BF16),
            pltpu.VMEM((256 * HEADS, 128), F32),
            pltpu.VMEM((2, 16, HEADS, 128), F32),
            pltpu.VMEM((ROWS, 256, TOK), F32),
            pltpu.VMEM((ROWS, 256, TOK), F32),
            pltpu.VMEM((3 * 128, 256, 128), BF16),
            pltpu.VMEM((HEADS, 8, TOK), F32),
            pltpu.VMEM((256, CH), BF16),
            pltpu.VMEM((256, CH), BF16),
            pltpu.VMEM((2, CH, TOK), F32),
            pltpu.SemaphoreType.DMA((NPIECES,)),
            pltpu.SemaphoreType.DMA((18,)),
            pltpu.SemaphoreType.DMA((18,)),
            pltpu.SemaphoreType.DMA((2, 19)),
            pltpu.SemaphoreType.DMA((2, 19)),
            pltpu.SemaphoreType.DMA((2, 15)),
            pltpu.SemaphoreType.DMA((2, 15)),
        ],
        compiler_params=pltpu.CompilerParams(
            collective_id=0, has_side_effects=True, vmem_limit_bytes=66_800_000
        ),
        name="pair_average",
    )(duo.reshape(128, 256, 128), w.T, msa, gain.reshape(1, CH), shift.reshape(1, CH), pw, sw, cw.T)


def solution(mesh):
    placed = (P("pi", "pj", None), P(), P("pj", None, "pi"), P(), P(), P(), P(), P())
    return jax.shard_map(
        body, mesh=mesh, in_specs=placed, out_specs=P("pj", None, "pi"), check_vma=False
    )
```

```python
import functools

import jax
import jax.numpy as jnp
from jax import lax
from jax.experimental import pallas as pl
from jax.experimental.pallas import tpu as pltpu
from jax.sharding import PartitionSpec as P

EPS = 1e-05
F32 = jnp.float32
BF16 = jnp.bfloat16
MESH = pl.DeviceIdType.MESH
NT = (((1,), (1,)), ((), ()))

HEADS = 8
SPAN = 32
ROWS = 32
CH = 64
TOK = 256
X_ROWS = 22
NPIECES = 8


def kernel(
    duo_hbm, wt_ref, msa_ref, gain_ref, shift_ref, pw_ref, sw_ref, cw_ref,
    out_ref,
    nbuf, ebuf, sc, mx, acc, gate, vbuf, tot, pwt, swt, gcol,
    duo_sem, n_send, n_recv, e_send, e_recv, m_send, m_recv,
):
    pi = lax.axis_index("pi")
    pj = lax.axis_index("pj")
    y, xl = lax.div(pi, 2), lax.rem(pi, 2)
    xh, zc = lax.div(pj, 8), lax.rem(pj, 8)
    z, core = lax.div(zc, 2), lax.rem(zc, 2)

    def pi_of(yy, ll):
        return yy * 2 + ll

    def pj_of(hh, zz, cc):
        return hh * 8 + zz * 2 + cc

    yp, ym, yo = lax.rem(y + 1, 4), lax.rem(y + 3, 4), lax.rem(y + 2, 4)
    zp, zm, zo = lax.rem(z + 1, 4), lax.rem(z + 3, 4), lax.rem(z + 2, 4)
    ol, oh = 1 - xl, 1 - xh
    y1, y3 = y + 1 - 2 * lax.rem(y, 2), 3 - y
    swap = lax.rem(lax.div(y, 2) + xh, 2)

    step = 128 // NPIECES

    def duo_copy(k):
        rows = pl.ds(k * step, step)
        there = pl.ds(256 + k * step, step)
        return pltpu.make_async_copy(duo_hbm.at[rows], vbuf.at[there], duo_sem.at[k])

    for k in range(NPIECES):
        duo_copy(k).start()

    barrier = pltpu.get_barrier_semaphore()
    for d in range(1, 16):
        pl.semaphore_signal(
            barrier, inc=1, device_id={"pi": pi, "pj": lax.rem(pj + d, 16)}, device_id_type=MESH
        )
    for other in (pi_of(yp, xl), pi_of(ym, xl), pi_of(y, ol)):
        pl.semaphore_signal(
            barrier, inc=1, device_id={"pi": other, "pj": pj}, device_id_type=MESH
        )

    def column(ref):
        row = jnp.broadcast_to(ref[...], (CH, CH))
        r = lax.broadcasted_iota(jnp.int32, (CH, CH), 0)
        c = lax.broadcasted_iota(jnp.int32, (CH, CH), 1)
        col = jnp.sum(jnp.where(r == c, row, 0.0), axis=1, keepdims=True)
        return jnp.broadcast_to(col, (CH, TOK))

    gcol[0] = column(gain_ref)
    gcol[1] = column(shift_ref)

    def norm_rows(g, _):
        for a in range(4):
            s = g * 4 + a
            v = msa_ref[s].astype(F32)
            mean = jnp.mean(v, axis=0, keepdims=True)
            v = v - mean
            var = jnp.mean(v * v, axis=0, keepdims=True)
            v = v * lax.rsqrt(var + EPS)
            nbuf[pi, s] = (v * gcol[0] + gcol[1]).astype(BF16)
        return 0

    lax.fori_loop(0, ROWS // 4, norm_rows, 0)
    pl.semaphore_wait(barrier, 18)

    xa, xb = X_ROWS // 2, X_ROWS
    ya, yb = X_ROWS + (ROWS - X_ROWS) // 2, ROWS

    def n_copy(k, block, lo, hi, to_y, to_l):
        view = nbuf.at[block, pl.ds(lo, hi - lo)]
        return pltpu.make_async_remote_copy(
            src_ref=view, dst_ref=view, send_sem=n_send.at[k], recv_sem=n_recv.at[k],
            device_id={"pi": pi_of(to_y, to_l), "pj": pj}, device_id_type=MESH,
        )

    own, part = pi, pi_of(y, ol)
    b_m, b_p, b_o = pi_of(ym, xl), pi_of(yp, xl), pi_of(yo, xl)
    q_m, q_p = pi_of(ym, ol), pi_of(yp, ol)
    n = [
        n_copy(0, own, 0, 6, y, ol),
        n_copy(1, own, xb, yb, y, ol),
        n_copy(2, own, xb, yb, yp, xl),
        n_copy(3, own, 0, xb, yp, xl),
        n_copy(4, own, xb, yb, ym, xl),
        n_copy(5, own, 0, xb, ym, xl),
        n_copy(6, b_m, xb, ya, yp, xl),
        n_copy(7, b_p, ya, yb, ym, xl),
        n_copy(8, pi_of(y3, xl), xb, yb, y, ol),
        n_copy(9, pi_of(y1, xl), xb, yb, y, ol),
        n_copy(10, b_o, xb, ya, y, ol),
        n_copy(11, b_o, ya, yb, y, ol),
        n_copy(12, part, 0, xb, yp, xl),
        n_copy(13, part, 0, xb, ym, xl),
        n_copy(14, b_m, 0, xa, yp, xl),
        n_copy(15, b_p, xa, xb, ym, xl),
        n_copy(16, q_m, 0, xa, yp, xl),
        n_copy(17, q_p, xa, xb, ym, xl),
        n_copy(18, own, 6, 14, y, ol),
        n_copy(19, own, 14, xb, y, ol),
    ]
    for k in (2, 4, 0, 3, 5):
        n[k].start()

    pwt[...] = pw_ref[...].astype(F32).T.astype(BF16)
    swt[...] = sw_ref[...].astype(F32).T.astype(BF16)

    w = wt_ref[...]
    w = w - jnp.mean(w, axis=1, keepdims=True)
    w_sum = jnp.sum(w, axis=1, keepdims=True)
    w_hi = w.astype(BF16)
    w_rest = w - w_hi.astype(F32)
    w_mid = w_rest.astype(BF16)
    w_lo = (w_rest - w_mid.astype(F32)).astype(BF16)
    ones8 = jnp.ones((8, 128), F32)
    stack = jnp.concatenate(
        [w_hi.astype(F32), w_mid.astype(F32), w_lo.astype(F32), ones8], axis=0
    ).astype(BF16)
    ones = jnp.ones((16, 128), BF16)
    group = 16

    def score_group(g, _):
        x = vbuf[pl.ds(256 + g * (group // 2), group // 2)].reshape(group * 128, 128)
        xf = x.astype(F32)
        sq = xf * xf
        sq_hi = sq.astype(BF16)
        sq_lo = (sq - sq_hi.astype(F32)).astype(BF16)
        r = lax.dot_general(stack, x, NT, preferred_element_type=F32)
        t_hi = lax.dot_general(ones, sq_hi, NT, preferred_element_type=F32)[0:8]
        t_lo = lax.dot_general(ones, sq_lo, NT, preferred_element_type=F32)[0:8]
        mean = r[24:32] * (1.0 / 128)
        m_hi = mean.astype(BF16).astype(F32)
        m_lo = mean - m_hi
        var = t_hi * (1.0 / 128) - m_hi * m_hi
        var = var - 2.0 * m_hi * m_lo
        var = (var - m_lo * m_lo) + t_lo * (1.0 / 128)
        var = jnp.maximum(var, 0.0)
        dots = (r[16:24] + r[8:16]) + r[0:8]
        s = (dots - mean * w_sum) * lax.rsqrt(var + EPS)
        for a in range(group):
            rows = pl.ds(pl.multiple_of((g * group + a) * 8, 8), 8)
            sc[rows, :] = s[:, a * 128:(a + 1) * 128]
        return 0

    per = 2 * step // group

    def score_piece(k, _):
        duo_copy(k).wait()
        lax.fori_loop(k * per, (k + 1) * per, score_group, 0)
        return 0

    def m_copy(r, d):
        view = mx.at[r, pj]
        return pltpu.make_async_remote_copy(
            src_ref=view, dst_ref=view, send_sem=m_send.at[r, d - 1],
            recv_sem=m_recv.at[r, d - 1],
            device_id={"pi": pi, "pj": lax.rem(pj + d, 16)}, device_id_type=MESH,
        )

    def scores_of(r):
        lax.fori_loop(r * NPIECES // 2, (r + 1) * NPIECES // 2, score_piece, 0)
        for h in range(HEADS):
            t = sc[pl.ds(r * 1024 + h, 128, stride=8), :].T
            acc[8 + h, 0:128, r * 128:(r + 1) * 128] = t
            mx[r, pj, pl.ds(h, 1), :] = jnp.max(t, axis=0, keepdims=True)
        for d in range(1, 16):
            m_copy(r, d).start()

    def columns(zz, cc):
        return pl.ds(pl.multiple_of(lax.rem(zz, 2) * 256 + cc * 128, 128), 128)

    def pair_of(hh, zz):
        return hh * 2 + lax.div(zz, 2)

    def exps_of(r):
        for d in range(1, 16):
            m_copy(r, d).wait_recv()
        peak = mx[r, 0]
        for d in range(1, 16):
            peak = jnp.maximum(peak, mx[r, d])
        lanes = slice(r * 128, (r + 1) * 128)
        for h in range(HEADS):
            t = jnp.exp(acc[8 + h, 0:128, lanes] - peak[h:h + 1])
            ebuf[pair_of(xh, z), h, columns(z, core), lanes] = t.astype(BF16)

    def e_copy(r, k, hh, zz, h0, h1, to_h, to_z, to_c):
        view = ebuf.at[
            pair_of(hh, zz), pl.ds(h0, h1 - h0), columns(zz, core), pl.ds(r * 128, 128)
        ]
        return pltpu.make_async_remote_copy(
            src_ref=view, dst_ref=view, send_sem=e_send.at[r, k], recv_sem=e_recv.at[r, k],
            device_id={"pi": pi, "pj": pj_of(to_h, to_z, to_c)}, device_id_type=MESH,
        )

    oc = 1 - core
    e = [
        [
            e_copy(r, 0, xh, z, 0, 8, xh, z, oc),
            e_copy(r, 1, xh, z, 0, 8, oh, z, core),
            e_copy(r, 2, xh, z, 0, 8, xh, zp, core),
            e_copy(r, 3, xh, z, 0, 8, xh, zm, core),
            e_copy(r, 4, oh, z, 0, 8, xh, zp, core),
            e_copy(r, 5, oh, z, 0, 8, xh, zm, core),
            e_copy(r, 6, oh, z, 0, 8, xh, z, oc),
            e_copy(r, 7, xh, zm, 0, 4, xh, zp, core),
            e_copy(r, 8, xh, zm, 0, 8, xh, z, oc),
            e_copy(r, 9, xh, zp, 4, 8, xh, zm, core),
            e_copy(r, 10, xh, zp, 0, 8, xh, z, oc),
            e_copy(r, 11, xh, zo, 0, 4, xh, z, oc),
            e_copy(r, 12, xh, zo, 4, 8, xh, z, oc),
            e_copy(r, 13, oh, zm, 0, 4, xh, zp, core),
            e_copy(r, 14, oh, zm, 0, 8, xh, z, oc),
            e_copy(r, 15, oh, zp, 4, 8, xh, zm, core),
            e_copy(r, 16, oh, zp, 0, 8, xh, z, oc),
            e_copy(r, 17, oh, zo, 0, 4, xh, z, oc),
            e_copy(r, 18, oh, zo, 4, 8, xh, z, oc),
        ]
        for r in range(2)
    ]

    def gate_rows(g, _):
        for a in range(4):
            s = g * 4 + a
            t = jnp.dot(swt[...], nbuf[pi, s], preferred_element_type=F32)
            gate[s] = jax.nn.sigmoid(t)
        return 0

    ones_t = jnp.ones((16, 2 * TOK), BF16)

    def value_rows(p, slot, c, g, _):
        for a in range(16):
            s = g * 16 + a
            v = jnp.dot(pwt[...], nbuf[p, s], preferred_element_type=F32).astype(BF16)
            vbuf[slot * 128 + s * 4 + c * 2] = v[:, 0:128]
            vbuf[slot * 128 + s * 4 + c * 2 + 1] = v[:, 128:256]
        return 0

    def head_step(yy, slot, g, _):
        v4 = vbuf.at[pl.ds(slot * 128, 128)]
        for a in range(2):
            h = g * 2 + a
            rows = pl.ds(pl.multiple_of(h * SPAN, SPAN), SPAN)
            weights = ebuf[yy, h]
            v = v4[:, rows, :].reshape(ROWS, 4, SPAN, 128)
            v = jnp.concatenate(
                [v[:, t].reshape(ROWS * SPAN, 128) for t in range(4)], axis=1
            )
            part_sum = jnp.dot(v, weights, preferred_element_type=F32)
            acc[:, rows, :] += part_sum.reshape(ROWS, SPAN, TOK)
            tot[h] += jnp.dot(ones_t, weights, preferred_element_type=F32)[0:8]
        return 0

    def values_of(p, slot, c):
        lax.fori_loop(0, ROWS // 16, functools.partial(value_rows, p, slot, c), 0)

    def product_of(yy, slot):
        lax.fori_loop(0, HEADS // 2, functools.partial(head_step, yy, slot), 0)

    def hop(r, k, *then):
        e[r][k].wait_recv()
        for t in then:
            e[r][t].start()

    scores_of(0)
    n[18].start()
    scores_of(1)
    exps_of(0)
    for k in (2, 3, 1, 0):
        e[0][k].start()
    n[19].start()
    n[2].wait_recv()
    n[6].start()
    n[4].wait_recv()
    n[7].start()
    lax.fori_loop(0, ROWS // 4, gate_rows, 0)
    exps_of(1)
    for k in (2, 3, 1, 0):
        e[1][k].start()
    for k in (1, 8, 9):
        n[k].start()
    acc[...] = jnp.zeros_like(acc)
    tot[...] = jnp.zeros_like(tot)
    values_of(own, 0, xl)
    hop(0, 2, 7, 8)
    hop(0, 3, 9, 10)
    for k in (0, 18, 19):
        n[k].wait_recv()
    n[12].start()
    n[13].start()
    hop(0, 1, 4, 5, 6)
    hop(1, 2, 7, 8)
    hop(1, 3, 9, 10)
    n[3].wait_recv()
    n[14].start()
    n[5].wait_recv()
    n[15].start()
    values_of(pi_of(y3, xl), 2, xl)
    hop(1, 1, 4, 5, 6)
    n[6].wait_recv()
    n[10].start()
    n[7].wait_recv()
    n[11].start()
    hop(0, 7, 11)
    hop(0, 9, 12)
    values_of(pi_of(y1, xl), 1, xl)
    hop(1, 7, 11)
    hop(1, 9, 12)
    n[1].wait_recv()
    values_of(part, 0, ol)
    hop(0, 4, 13, 14)
    hop(0, 5, 15, 16)
    hop(1, 4, 13, 14)
    hop(1, 5, 15, 16)
    n[12].wait_recv()
    n[16].start()
    n[13].wait_recv()
    n[17].start()
    n[8].wait_recv()
    values_of(pi_of(y3, ol), 2, ol)
    for r in range(2):
        for k in (0, 8, 10, 11, 12):
            e[r][k].wait_recv()
    product_of(y * (1 - swap) + y3 * swap, 2 * swap)
    for r in range(2):
        hop(r, 13, 17)
        hop(r, 15, 18)
    for r in range(2):
        for k in (6, 14, 16, 17, 18):
            e[r][k].wait_recv()
    product_of(y3 * (1 - swap) + y * swap, 2 - 2 * swap)
    n[9].wait_recv()
    values_of(pi_of(y1, ol), 1, ol)
    product_of(y1, 1)
    n[14].wait_recv()
    n[15].wait_recv()
    values_of(b_o, 2 * swap, xl)
    for k in (10, 11, 16, 17):
        n[k].wait_recv()
    values_of(pi_of(yo, ol), 2 * swap, ol)
    product_of(yo, 2 * swap)

    for h in range(HEADS):
        tot[h] = 1.0 / tot[h]

    def out_rows(g, _):
        for a in range(4):
            s = g * 4 + a
            pieces = []
            for h in range(HEADS):
                rows = slice(h * SPAN, (h + 1) * SPAN)
                share = tot[h, 0:1, :]
                pieces.append((gate[s, rows, :] * (acc[s, rows, :] * share)).astype(BF16))
            mixed = jnp.concatenate(pieces, axis=0)
            out_ref[s] = jnp.dot(cw_ref[...], mixed, preferred_element_type=F32).astype(BF16)
        return 0

    lax.fori_loop(0, ROWS // 4, out_rows, 0)

    for c in n + e[0] + e[1]:
        c.wait_send()
    for r in range(2):
        for d in range(1, 16):
            m_copy(r, d).wait_send()


def body(duo, w, msa, gain, shift, pw, sw, cw):
    vm = pl.BlockSpec(memory_space=pltpu.VMEM)
    return pl.pallas_call(
        kernel,
        out_shape=jax.ShapeDtypeStruct((ROWS, CH, TOK), BF16),
        in_specs=[pl.BlockSpec(memory_space=pl.ANY)] + [vm] * 7,
        out_specs=vm,
        scratch_shapes=[
            pltpu.VMEM((8, ROWS, CH, TOK), BF16),
            pltpu.VMEM((4, HEADS, 2 * TOK, TOK), BF16),
            pltpu.VMEM((256 * HEADS, 128), F32),
            pltpu.VMEM((2, 16, HEADS, 128), F32),
            pltpu.VMEM((ROWS, 256, TOK), F32),
            pltpu.VMEM((ROWS, 256, TOK), F32),
            pltpu.VMEM((3 * 128, 256, 128), BF16),
            pltpu.VMEM((HEADS, 8, TOK), F32),
            pltpu.VMEM((256, CH), BF16),
            pltpu.VMEM((256, CH), BF16),
            pltpu.VMEM((2, CH, TOK), F32),
            pltpu.SemaphoreType.DMA((NPIECES,)),
            pltpu.SemaphoreType.DMA((20,)),
            pltpu.SemaphoreType.DMA((20,)),
            pltpu.SemaphoreType.DMA((2, 19)),
            pltpu.SemaphoreType.DMA((2, 19)),
            pltpu.SemaphoreType.DMA((2, 15)),
            pltpu.SemaphoreType.DMA((2, 15)),
        ],
        compiler_params=pltpu.CompilerParams(
            collective_id=0, has_side_effects=True, vmem_limit_bytes=66_800_000
        ),
        name="pair_average",
    )(duo.reshape(128, 256, 128), w.T, msa, gain.reshape(1, CH), shift.reshape(1, CH), pw, sw, cw.T)


def solution(mesh):
    placed = (P("pi", "pj", None), P(), P("pj", None, "pi"), P(), P(), P(), P(), P())
    return jax.shard_map(
        body, mesh=mesh, in_specs=placed, out_specs=P("pj", None, "pi"), check_vma=False
    )
```

```python
import functools

import jax
import jax.numpy as jnp
from jax import lax
from jax.experimental import pallas as pl
from jax.experimental.pallas import tpu as pltpu
from jax.sharding import PartitionSpec as P

EPS = 1e-05
F32 = jnp.float32
BF16 = jnp.bfloat16
MESH = pl.DeviceIdType.MESH
NT = (((1,), (1,)), ((), ()))

HEADS = 8
SPAN = 32
ROWS = 32
CH = 64
TOK = 256
X_ROWS = 21
NPIECES = 8
H_UNROLL = 8


def kernel(
    duo_hbm, wt_ref, msa_ref, gain_ref, shift_ref, pw_ref, sw_ref, cw_ref,
    out_ref,
    nbuf, ebuf, sc, mx, acc, gate, vbuf, tot, pwt, swt, gcol,
    duo_sem, n_send, n_recv, e_send, e_recv, m_send, m_recv,
):
    pi = lax.axis_index("pi")
    pj = lax.axis_index("pj")
    y, xl = lax.div(pi, 2), lax.rem(pi, 2)
    xh, zc = lax.div(pj, 8), lax.rem(pj, 8)
    z, core = lax.div(zc, 2), lax.rem(zc, 2)

    def pi_of(yy, ll):
        return yy * 2 + ll

    def pj_of(hh, zz, cc):
        return hh * 8 + zz * 2 + cc

    yp, ym, yo = lax.rem(y + 1, 4), lax.rem(y + 3, 4), lax.rem(y + 2, 4)
    zp, zm, zo = lax.rem(z + 1, 4), lax.rem(z + 3, 4), lax.rem(z + 2, 4)
    ol, oh = 1 - xl, 1 - xh
    y1, y3 = y + 1 - 2 * lax.rem(y, 2), 3 - y
    swap = lax.rem(lax.div(y, 2) + xh, 2)

    step = 128 // NPIECES

    def duo_copy(k):
        rows = pl.ds(k * step, step)
        there = pl.ds(256 + k * step, step)
        return pltpu.make_async_copy(duo_hbm.at[rows], vbuf.at[there], duo_sem.at[k])

    for k in range(NPIECES):
        duo_copy(k).start()

    barrier = pltpu.get_barrier_semaphore()
    for d in range(1, 16):
        pl.semaphore_signal(
            barrier, inc=1, device_id={"pi": pi, "pj": lax.rem(pj + d, 16)}, device_id_type=MESH
        )
    for other in (pi_of(yp, xl), pi_of(ym, xl), pi_of(y, ol)):
        pl.semaphore_signal(
            barrier, inc=1, device_id={"pi": other, "pj": pj}, device_id_type=MESH
        )

    def column(ref):
        row = jnp.broadcast_to(ref[...], (CH, CH))
        r = lax.broadcasted_iota(jnp.int32, (CH, CH), 0)
        c = lax.broadcasted_iota(jnp.int32, (CH, CH), 1)
        col = jnp.sum(jnp.where(r == c, row, 0.0), axis=1, keepdims=True)
        return jnp.broadcast_to(col, (CH, TOK))

    gcol[0] = column(gain_ref)
    gcol[1] = column(shift_ref)

    def norm_rows(g, _):
        for a in range(4):
            s = g * 4 + a
            v = msa_ref[s].astype(F32)
            mean = jnp.mean(v, axis=0, keepdims=True)
            v = v - mean
            var = jnp.mean(v * v, axis=0, keepdims=True)
            v = v * lax.rsqrt(var + EPS)
            nbuf[pi, s] = (v * gcol[0] + gcol[1]).astype(BF16)
        return 0

    lax.fori_loop(0, ROWS // 4, norm_rows, 0)
    pl.semaphore_wait(barrier, 18)

    xa, xb = X_ROWS // 2, X_ROWS
    ya, yb = X_ROWS + (ROWS - X_ROWS) // 2, ROWS

    def n_copy(k, block, lo, hi, to_y, to_l):
        view = nbuf.at[block, pl.ds(lo, hi - lo)]
        return pltpu.make_async_remote_copy(
            src_ref=view, dst_ref=view, send_sem=n_send.at[k], recv_sem=n_recv.at[k],
            device_id={"pi": pi_of(to_y, to_l), "pj": pj}, device_id_type=MESH,
        )

    own, part = pi, pi_of(y, ol)
    b_m, b_p, b_o = pi_of(ym, xl), pi_of(yp, xl), pi_of(yo, xl)
    q_m, q_p = pi_of(ym, ol), pi_of(yp, ol)
    n = [
        n_copy(0, own, 0, 6, y, ol),
        n_copy(1, own, xb, yb, y, ol),
        n_copy(2, own, xb, yb, yp, xl),
        n_copy(3, own, 0, xb, yp, xl),
        n_copy(4, own, xb, yb, ym, xl),
        n_copy(5, own, 0, xb, ym, xl),
        n_copy(6, b_m, xb, ya, yp, xl),
        n_copy(7, b_p, ya, yb, ym, xl),
        n_copy(8, pi_of(y3, xl), xb, yb, y, ol),
        n_copy(9, pi_of(y1, xl), xb, yb, y, ol),
        n_copy(10, b_o, xb, ya, y, ol),
        n_copy(11, b_o, ya, yb, y, ol),
        n_copy(12, part, 0, xb, yp, xl),
        n_copy(13, part, 0, xb, ym, xl),
        n_copy(14, b_m, 0, xa, yp, xl),
        n_copy(15, b_p, xa, xb, ym, xl),
        n_copy(16, q_m, 0, xa, yp, xl),
        n_copy(17, q_p, xa, xb, ym, xl),
        n_copy(18, own, 6, 14, y, ol),
        n_copy(19, own, 14, xb, y, ol),
    ]
    for k in (2, 4, 0, 3, 5):
        n[k].start()

    pwt[...] = pw_ref[...].astype(F32).T.astype(BF16)
    swt[...] = sw_ref[...].astype(F32).T.astype(BF16)

    w = wt_ref[...]
    w = w - jnp.mean(w, axis=1, keepdims=True)
    w_sum = jnp.sum(w, axis=1, keepdims=True)
    w_hi = w.astype(BF16)
    w_rest = w - w_hi.astype(F32)
    w_mid = w_rest.astype(BF16)
    w_lo = (w_rest - w_mid.astype(F32)).astype(BF16)
    ones8 = jnp.ones((8, 128), F32)
    stack = jnp.concatenate(
        [w_hi.astype(F32), w_mid.astype(F32), w_lo.astype(F32), ones8], axis=0
    ).astype(BF16)
    ones = jnp.ones((16, 128), BF16)
    group = 16

    def score_group(g, _):
        x = vbuf[pl.ds(256 + g * (group // 2), group // 2)].reshape(group * 128, 128)
        xf = x.astype(F32)
        sq = xf * xf
        sq_hi = sq.astype(BF16)
        sq_lo = (sq - sq_hi.astype(F32)).astype(BF16)
        r = lax.dot_general(stack, x, NT, preferred_element_type=F32)
        t_hi = lax.dot_general(ones, sq_hi, NT, preferred_element_type=F32)[0:8]
        t_lo = lax.dot_general(ones, sq_lo, NT, preferred_element_type=F32)[0:8]
        mean = r[24:32] * (1.0 / 128)
        m_hi = mean.astype(BF16).astype(F32)
        m_lo = mean - m_hi
        var = t_hi * (1.0 / 128) - m_hi * m_hi
        var = var - 2.0 * m_hi * m_lo
        var = (var - m_lo * m_lo) + t_lo * (1.0 / 128)
        var = jnp.maximum(var, 0.0)
        dots = (r[16:24] + r[8:16]) + r[0:8]
        s = (dots - mean * w_sum) * lax.rsqrt(var + EPS)
        for a in range(group):
            rows = pl.ds(pl.multiple_of((g * group + a) * 8, 8), 8)
            sc[rows, :] = s[:, a * 128:(a + 1) * 128]
        return 0

    per = 2 * step // group

    def score_piece(k, _):
        duo_copy(k).wait()
        lax.fori_loop(k * per, (k + 1) * per, score_group, 0)
        return 0

    def m_copy(r, d):
        view = mx.at[r, pj]
        return pltpu.make_async_remote_copy(
            src_ref=view, dst_ref=view, send_sem=m_send.at[r, d - 1],
            recv_sem=m_recv.at[r, d - 1],
            device_id={"pi": pi, "pj": lax.rem(pj + d, 16)}, device_id_type=MESH,
        )

    def scores_of(r):
        lax.fori_loop(r * NPIECES // 2, (r + 1) * NPIECES // 2, score_piece, 0)
        for h in range(HEADS):
            t = sc[pl.ds(r * 1024 + h, 128, stride=8), :].T
            acc[8 + h, 0:128, r * 128:(r + 1) * 128] = t
            mx[r, pj, pl.ds(h, 1), :] = jnp.max(t, axis=0, keepdims=True)
        for d in range(1, 16):
            m_copy(r, d).start()

    def columns(zz, cc):
        return pl.ds(pl.multiple_of(lax.rem(zz, 2) * 256 + cc * 128, 128), 128)

    def pair_of(hh, zz):
        return hh * 2 + lax.div(zz, 2)

    def exps_of(r):
        for d in range(1, 16):
            m_copy(r, d).wait_recv()
        peak = mx[r, 0]
        for d in range(1, 16):
            peak = jnp.maximum(peak, mx[r, d])
        lanes = slice(r * 128, (r + 1) * 128)
        for h in range(HEADS):
            t = jnp.exp(acc[8 + h, 0:128, lanes] - peak[h:h + 1])
            ebuf[pair_of(xh, z), h, columns(z, core), lanes] = t.astype(BF16)

    def e_copy(r, k, hh, zz, h0, h1, to_h, to_z, to_c):
        view = ebuf.at[
            pair_of(hh, zz), pl.ds(h0, h1 - h0), columns(zz, core), pl.ds(r * 128, 128)
        ]
        return pltpu.make_async_remote_copy(
            src_ref=view, dst_ref=view, send_sem=e_send.at[r, k], recv_sem=e_recv.at[r, k],
            device_id={"pi": pi, "pj": pj_of(to_h, to_z, to_c)}, device_id_type=MESH,
        )

    oc = 1 - core
    e = [
        [
            e_copy(r, 0, xh, z, 0, 8, xh, z, oc),
            e_copy(r, 1, xh, z, 0, 8, oh, z, core),
            e_copy(r, 2, xh, z, 0, 8, xh, zp, core),
            e_copy(r, 3, xh, z, 0, 8, xh, zm, core),
            e_copy(r, 4, oh, z, 0, 8, xh, zp, core),
            e_copy(r, 5, oh, z, 0, 8, xh, zm, core),
            e_copy(r, 6, oh, z, 0, 8, xh, z, oc),
            e_copy(r, 7, xh, zm, 0, 4, xh, zp, core),
            e_copy(r, 8, xh, zm, 0, 8, xh, z, oc),
            e_copy(r, 9, xh, zp, 4, 8, xh, zm, core),
            e_copy(r, 10, xh, zp, 0, 8, xh, z, oc),
            e_copy(r, 11, xh, zo, 0, 4, xh, z, oc),
            e_copy(r, 12, xh, zo, 4, 8, xh, z, oc),
            e_copy(r, 13, oh, zm, 0, 4, xh, zp, core),
            e_copy(r, 14, oh, zm, 0, 8, xh, z, oc),
            e_copy(r, 15, oh, zp, 4, 8, xh, zm, core),
            e_copy(r, 16, oh, zp, 0, 8, xh, z, oc),
            e_copy(r, 17, oh, zo, 0, 4, xh, z, oc),
            e_copy(r, 18, oh, zo, 4, 8, xh, z, oc),
        ]
        for r in range(2)
    ]

    def gate_rows(g, _):
        for a in range(4):
            s = g * 4 + a
            t = jnp.dot(swt[...], nbuf[pi, s], preferred_element_type=F32)
            gate[s] = jax.nn.sigmoid(t)
        return 0

    mine, other = pl.multiple_of(xl * TOK, TOK), pl.multiple_of(ol * TOK, TOK)

    def value_rows(p, slot, c, g, _):
        for a in range(16):
            s = g * 16 + a
            v = jnp.dot(pwt[...], nbuf[p, s], preferred_element_type=F32).astype(BF16)
            vbuf[slot * 128 + s * 4 + c * 2] = v[:, 0:128]
            vbuf[slot * 128 + s * 4 + c * 2 + 1] = v[:, 128:256]
        return 0

    def head_step(yy, slot, classes, g, _):
        v4 = vbuf.at[pl.ds(slot * 128, 128)]
        depth = len(classes) * TOK
        for a in range(H_UNROLL):
            h = g * H_UNROLL + a
            rows = pl.ds(pl.multiple_of(h * SPAN, SPAN), SPAN)
            weights = [ebuf[yy, h, pl.ds((mine, other)[c], TOK), :] for c in classes]
            weights = weights[0] if len(classes) == 1 else jnp.concatenate(weights, axis=0)
            v = v4[:, rows, :].reshape(ROWS, 4, SPAN, 128)
            v = jnp.concatenate(
                [v[:, 2 * c + t].reshape(ROWS * SPAN, 128) for c in classes for t in range(2)],
                axis=1,
            )
            v = jnp.concatenate([v, jnp.ones((16, depth), BF16)], axis=0)
            part_sum = jnp.dot(v, weights, preferred_element_type=F32)
            acc[:, rows, :] += part_sum[:ROWS * SPAN].reshape(ROWS, SPAN, TOK)
            tot[h] += part_sum[ROWS * SPAN:ROWS * SPAN + 8]
        return 0

    def values_of(p, slot, c):
        lax.fori_loop(0, ROWS // 16, functools.partial(value_rows, p, slot, c), 0)

    def product_of(yy, slot, classes=(0, 1)):
        step = functools.partial(head_step, yy, slot, classes)
        lax.fori_loop(0, HEADS // H_UNROLL, step, 0)

    def hop(r, k, *then):
        e[r][k].wait_recv()
        for t in then:
            e[r][t].start()

    scores_of(0)
    n[18].start()
    scores_of(1)
    exps_of(0)
    for k in (2, 3, 1, 0):
        e[0][k].start()
    n[19].start()
    n[2].wait_recv()
    n[6].start()
    n[4].wait_recv()
    n[7].start()
    lax.fori_loop(0, ROWS // 4, gate_rows, 0)
    exps_of(1)
    for k in (2, 3, 1, 0):
        e[1][k].start()
    for k in (1, 8, 9):
        n[k].start()
    acc[...] = jnp.zeros_like(acc)
    tot[...] = jnp.zeros_like(tot)
    values_of(own, 0, 0)
    hop(0, 2, 7, 8)
    hop(0, 3, 9, 10)
    for k in (0, 18, 19):
        n[k].wait_recv()
    n[12].start()
    n[13].start()
    hop(0, 1, 4, 5, 6)
    hop(1, 2, 7, 8)
    hop(1, 3, 9, 10)
    n[3].wait_recv()
    n[14].start()
    n[5].wait_recv()
    n[15].start()
    values_of(pi_of(y3, xl), 2, 0)
    hop(1, 1, 4, 5, 6)
    n[6].wait_recv()
    n[10].start()
    n[7].wait_recv()
    n[11].start()
    hop(0, 7, 11)
    hop(0, 9, 12)
    values_of(pi_of(y1, xl), 1, 0)
    hop(1, 7, 11)
    hop(1, 9, 12)
    n[1].wait_recv()
    values_of(part, 0, 1)
    hop(0, 4, 13, 14)
    hop(0, 5, 15, 16)
    for r in range(2):
        for k in (0, 8, 10, 11, 12):
            e[r][k].wait_recv()
    product_of(y * (1 - swap) + y3 * swap, 2 * swap, (0,))
    hop(1, 4, 13, 14)
    hop(1, 5, 15, 16)
    n[12].wait_recv()
    n[16].start()
    n[13].wait_recv()
    n[17].start()
    n[8].wait_recv()
    values_of(pi_of(y3, ol), 2, 1)
    product_of(y * (1 - swap) + y3 * swap, 2 * swap, (1,))
    for r in range(2):
        hop(r, 13, 17)
        hop(r, 15, 18)
    for r in range(2):
        for k in (6, 14, 16, 17, 18):
            e[r][k].wait_recv()
    product_of(y3 * (1 - swap) + y * swap, 2 - 2 * swap)
    n[9].wait_recv()
    values_of(pi_of(y1, ol), 1, 1)
    product_of(y1, 1)
    n[14].wait_recv()
    n[15].wait_recv()
    values_of(b_o, 2 * swap, 0)
    product_of(yo, 2 * swap, (0,))
    for k in (10, 11, 16, 17):
        n[k].wait_recv()
    values_of(pi_of(yo, ol), 2 * swap, 1)
    product_of(yo, 2 * swap, (1,))

    for h in range(HEADS):
        tot[h] = 1.0 / tot[h]

    def out_rows(g, _):
        for a in range(8):
            s = g * 8 + a
            pieces = []
            for h in range(HEADS):
                rows = slice(h * SPAN, (h + 1) * SPAN)
                share = tot[h, 0:1, :]
                pieces.append((gate[s, rows, :] * (acc[s, rows, :] * share)).astype(BF16))
            mixed = jnp.concatenate(pieces, axis=0)
            out_ref[s] = jnp.dot(cw_ref[...], mixed, preferred_element_type=F32).astype(BF16)
        return 0

    lax.fori_loop(0, ROWS // 8, out_rows, 0)

    for c in n + e[0] + e[1]:
        c.wait_send()
    for r in range(2):
        for d in range(1, 16):
            m_copy(r, d).wait_send()


def body(duo, w, msa, gain, shift, pw, sw, cw):
    vm = pl.BlockSpec(memory_space=pltpu.VMEM)
    return pl.pallas_call(
        kernel,
        out_shape=pltpu.VMEM((ROWS, CH, TOK), BF16),
        in_specs=[pl.BlockSpec(memory_space=pl.ANY)] + [vm] * 7,
        out_specs=vm,
        scratch_shapes=[
            pltpu.VMEM((8, ROWS, CH, TOK), BF16),
            pltpu.VMEM((4, HEADS, 2 * TOK, TOK), BF16),
            pltpu.VMEM((256 * HEADS, 128), F32),
            pltpu.VMEM((2, 16, HEADS, 128), F32),
            pltpu.VMEM((ROWS, 256, TOK), F32),
            pltpu.VMEM((ROWS, 256, TOK), F32),
            pltpu.VMEM((3 * 128, 256, 128), BF16),
            pltpu.VMEM((HEADS, 8, TOK), F32),
            pltpu.VMEM((256, CH), BF16),
            pltpu.VMEM((256, CH), BF16),
            pltpu.VMEM((2, CH, TOK), F32),
            pltpu.SemaphoreType.DMA((NPIECES,)),
            pltpu.SemaphoreType.DMA((20,)),
            pltpu.SemaphoreType.DMA((20,)),
            pltpu.SemaphoreType.DMA((2, 19)),
            pltpu.SemaphoreType.DMA((2, 19)),
            pltpu.SemaphoreType.DMA((2, 15)),
            pltpu.SemaphoreType.DMA((2, 15)),
        ],
        compiler_params=pltpu.CompilerParams(
            collective_id=0, has_side_effects=True, vmem_limit_bytes=65_000_000
        ),
        name="pair_average",
    )(duo.reshape(128, 256, 128), w.T, msa, gain.reshape(1, CH), shift.reshape(1, CH), pw, sw, cw.T)


def solution(mesh):
    placed = (P("pi", "pj", None), P(), P("pj", None, "pi"), P(), P(), P(), P(), P())
    return jax.shard_map(
        body, mesh=mesh, in_specs=placed, out_specs=P("pj", None, "pi"), check_vma=False
    )
```

```python
import functools

import jax
import jax.numpy as jnp
from jax import lax
from jax.experimental import pallas as pl
from jax.experimental.pallas import tpu as pltpu
from jax.sharding import PartitionSpec as P

EPS = 1e-05
F32 = jnp.float32
BF16 = jnp.bfloat16
MESH = pl.DeviceIdType.MESH
NT = (((1,), (1,)), ((), ()))

HEADS = 8
SPAN = 32
ROWS = 32
CH = 64
TOK = 256
X_ROWS = 21
NPIECES = 8
H_UNROLL = 8


def kernel(
    duo_hbm, wt_ref, msa_hbm, gain_ref, shift_ref, pw_ref, sw_ref, cw_ref,
    out_ref,
    msa, nbuf, ebuf, sc, mx, acc, gate, vbuf, tot, pwt, swt, gcol,
    msa_sem, duo_sem, n_send, n_recv, e_send, e_recv, m_send, m_recv,
):
    pi = lax.axis_index("pi")
    pj = lax.axis_index("pj")
    y, xl = lax.div(pi, 2), lax.rem(pi, 2)
    xh, zc = lax.div(pj, 8), lax.rem(pj, 8)
    z, core = lax.div(zc, 2), lax.rem(zc, 2)

    def pi_of(yy, ll):
        return yy * 2 + ll

    def pj_of(hh, zz, cc):
        return hh * 8 + zz * 2 + cc

    yp, ym, yo = lax.rem(y + 1, 4), lax.rem(y + 3, 4), lax.rem(y + 2, 4)
    zp, zm, zo = lax.rem(z + 1, 4), lax.rem(z + 3, 4), lax.rem(z + 2, 4)
    ol, oh = 1 - xl, 1 - xh
    y1, y3 = y + 1 - 2 * lax.rem(y, 2), 3 - y
    swap = lax.rem(lax.div(y, 2) + xh, 2)

    def msa_copy(k, lo, hi):
        rows = pl.ds(lo, hi - lo)
        return pltpu.make_async_copy(msa_hbm.at[rows], msa.at[rows], msa_sem.at[k])

    msa_in = [msa_copy(0, X_ROWS, ROWS), msa_copy(1, 0, X_ROWS)]
    for c in msa_in:
        c.start()

    step = 128 // NPIECES

    def duo_copy(k):
        rows = pl.ds(k * step, step)
        there = pl.ds(256 + k * step, step)
        return pltpu.make_async_copy(duo_hbm.at[rows], vbuf.at[there], duo_sem.at[k])

    barrier = pltpu.get_barrier_semaphore()
    for d in range(1, 16):
        pl.semaphore_signal(
            barrier, inc=1, device_id={"pi": pi, "pj": lax.rem(pj + d, 16)}, device_id_type=MESH
        )
    for other in (pi_of(yp, xl), pi_of(ym, xl), pi_of(y, ol)):
        pl.semaphore_signal(
            barrier, inc=1, device_id={"pi": other, "pj": pj}, device_id_type=MESH
        )

    for k in range(NPIECES):
        duo_copy(k).start()

    def column(ref):
        row = jnp.broadcast_to(ref[...], (CH, CH))
        r = lax.broadcasted_iota(jnp.int32, (CH, CH), 0)
        c = lax.broadcasted_iota(jnp.int32, (CH, CH), 1)
        col = jnp.sum(jnp.where(r == c, row, 0.0), axis=1, keepdims=True)
        return jnp.broadcast_to(col, (CH, TOK))

    gcol[0] = column(gain_ref)
    gcol[1] = column(shift_ref)

    def norm_range(lo, hi):
        for s in range(lo, hi):
            v = msa[s].astype(F32)
            mean = jnp.mean(v, axis=0, keepdims=True)
            v = v - mean
            var = jnp.mean(v * v, axis=0, keepdims=True)
            v = v * lax.rsqrt(var + EPS)
            nbuf[pi, s] = (v * gcol[0] + gcol[1]).astype(BF16)

    xa, xb = X_ROWS // 2, X_ROWS
    ya, yb = X_ROWS + (ROWS - X_ROWS) // 2, ROWS

    def n_copy(k, block, lo, hi, to_y, to_l):
        view = nbuf.at[block, pl.ds(lo, hi - lo)]
        return pltpu.make_async_remote_copy(
            src_ref=view, dst_ref=view, send_sem=n_send.at[k], recv_sem=n_recv.at[k],
            device_id={"pi": pi_of(to_y, to_l), "pj": pj}, device_id_type=MESH,
        )

    own, part = pi, pi_of(y, ol)
    b_m, b_p, b_o = pi_of(ym, xl), pi_of(yp, xl), pi_of(yo, xl)
    q_m, q_p = pi_of(ym, ol), pi_of(yp, ol)
    n = [
        n_copy(0, own, 0, 6, y, ol),
        n_copy(1, own, xb, yb, y, ol),
        n_copy(2, own, xb, yb, yp, xl),
        n_copy(3, own, 0, xb, yp, xl),
        n_copy(4, own, xb, yb, ym, xl),
        n_copy(5, own, 0, xb, ym, xl),
        n_copy(6, b_m, xb, ya, yp, xl),
        n_copy(7, b_p, ya, yb, ym, xl),
        n_copy(8, pi_of(y3, xl), xb, yb, y, ol),
        n_copy(9, pi_of(y1, xl), xb, yb, y, ol),
        n_copy(10, b_o, xb, ya, y, ol),
        n_copy(11, b_o, ya, yb, y, ol),
        n_copy(12, part, 0, xb, yp, xl),
        n_copy(13, part, 0, xb, ym, xl),
        n_copy(14, b_m, 0, xa, yp, xl),
        n_copy(15, b_p, xa, xb, ym, xl),
        n_copy(16, q_m, 0, xa, yp, xl),
        n_copy(17, q_p, xa, xb, ym, xl),
        n_copy(18, own, 6, 14, y, ol),
        n_copy(19, own, 14, xb, y, ol),
    ]
    msa_in[0].wait()
    norm_range(X_ROWS, ROWS)
    pl.semaphore_wait(barrier, 18)
    for k in (2, 4):
        n[k].start()
    msa_in[1].wait()
    norm_range(0, 6)
    n[0].start()
    norm_range(6, X_ROWS)
    for k in (3, 5):
        n[k].start()

    pwt[...] = pw_ref[...].astype(F32).T.astype(BF16)
    swt[...] = sw_ref[...].astype(F32).T.astype(BF16)

    w = wt_ref[...]
    w = w - jnp.mean(w, axis=1, keepdims=True)
    w_sum = jnp.sum(w, axis=1, keepdims=True)
    w_hi = w.astype(BF16)
    w_rest = w - w_hi.astype(F32)
    w_mid = w_rest.astype(BF16)
    w_lo = (w_rest - w_mid.astype(F32)).astype(BF16)
    ones8 = jnp.ones((8, 128), F32)
    stack = jnp.concatenate(
        [w_hi.astype(F32), w_mid.astype(F32), w_lo.astype(F32), ones8], axis=0
    ).astype(BF16)
    ones = jnp.ones((16, 128), BF16)
    group = 16

    def score_group(g, _):
        x = vbuf[pl.ds(256 + g * (group // 2), group // 2)].reshape(group * 128, 128)
        xf = x.astype(F32)
        sq = xf * xf
        sq_hi = sq.astype(BF16)
        sq_lo = (sq - sq_hi.astype(F32)).astype(BF16)
        r = lax.dot_general(stack, x, NT, preferred_element_type=F32)
        t_hi = lax.dot_general(ones, sq_hi, NT, preferred_element_type=F32)[0:8]
        t_lo = lax.dot_general(ones, sq_lo, NT, preferred_element_type=F32)[0:8]
        mean = r[24:32] * (1.0 / 128)
        m_hi = mean.astype(BF16).astype(F32)
        m_lo = mean - m_hi
        var = t_hi * (1.0 / 128) - m_hi * m_hi
        var = var - 2.0 * m_hi * m_lo
        var = (var - m_lo * m_lo) + t_lo * (1.0 / 128)
        var = jnp.maximum(var, 0.0)
        dots = (r[16:24] + r[8:16]) + r[0:8]
        s = (dots - mean * w_sum) * lax.rsqrt(var + EPS)
        for a in range(group):
            rows = pl.ds(pl.multiple_of((g * group + a) * 8, 8), 8)
            sc[rows, :] = s[:, a * 128:(a + 1) * 128]
        return 0

    per = 2 * step // group

    def score_piece(k, _):
        duo_copy(k).wait()
        lax.fori_loop(k * per, (k + 1) * per, score_group, 0)
        return 0

    def m_copy(r, d):
        view = mx.at[r, pj]
        return pltpu.make_async_remote_copy(
            src_ref=view, dst_ref=view, send_sem=m_send.at[r, d - 1],
            recv_sem=m_recv.at[r, d - 1],
            device_id={"pi": pi, "pj": lax.rem(pj + d, 16)}, device_id_type=MESH,
        )

    def scores_of(r):
        lax.fori_loop(r * NPIECES // 2, (r + 1) * NPIECES // 2, score_piece, 0)
        for h in range(HEADS):
            t = sc[pl.ds(r * 1024 + h, 128, stride=8), :].T
            acc[8 + h, 0:128, r * 128:(r + 1) * 128] = t
            mx[r, pj, pl.ds(h, 1), :] = jnp.max(t, axis=0, keepdims=True)
        for d in range(1, 16):
            m_copy(r, d).start()

    def columns(zz, cc):
        return pl.ds(pl.multiple_of(lax.rem(zz, 2) * 256 + cc * 128, 128), 128)

    def pair_of(hh, zz):
        return hh * 2 + lax.div(zz, 2)

    def exps_of(r):
        for d in range(1, 16):
            m_copy(r, d).wait_recv()
        peak = mx[r, 0]
        for d in range(1, 16):
            peak = jnp.maximum(peak, mx[r, d])
        lanes = slice(r * 128, (r + 1) * 128)
        for h in range(HEADS):
            t = jnp.exp(acc[8 + h, 0:128, lanes] - peak[h:h + 1])
            ebuf[pair_of(xh, z), h, columns(z, core), lanes] = t.astype(BF16)

    def e_copy(r, k, hh, zz, h0, h1, to_h, to_z, to_c):
        view = ebuf.at[
            pair_of(hh, zz), pl.ds(h0, h1 - h0), columns(zz, core), pl.ds(r * 128, 128)
        ]
        return pltpu.make_async_remote_copy(
            src_ref=view, dst_ref=view, send_sem=e_send.at[r, k], recv_sem=e_recv.at[r, k],
            device_id={"pi": pi, "pj": pj_of(to_h, to_z, to_c)}, device_id_type=MESH,
        )

    oc = 1 - core
    e = [
        [
            e_copy(r, 0, xh, z, 0, 8, xh, z, oc),
            e_copy(r, 1, xh, z, 0, 8, oh, z, core),
            e_copy(r, 2, xh, z, 0, 8, xh, zp, core),
            e_copy(r, 3, xh, z, 0, 8, xh, zm, core),
            e_copy(r, 4, oh, z, 0, 8, xh, zp, core),
            e_copy(r, 5, oh, z, 0, 8, xh, zm, core),
            e_copy(r, 6, oh, z, 0, 8, xh, z, oc),
            e_copy(r, 7, xh, zm, 0, 4, xh, zp, core),
            e_copy(r, 8, xh, zm, 0, 8, xh, z, oc),
            e_copy(r, 9, xh, zp, 4, 8, xh, zm, core),
            e_copy(r, 10, xh, zp, 0, 8, xh, z, oc),
            e_copy(r, 11, xh, zo, 0, 4, xh, z, oc),
            e_copy(r, 12, xh, zo, 4, 8, xh, z, oc),
            e_copy(r, 13, oh, zm, 0, 4, xh, zp, core),
            e_copy(r, 14, oh, zm, 0, 8, xh, z, oc),
            e_copy(r, 15, oh, zp, 4, 8, xh, zm, core),
            e_copy(r, 16, oh, zp, 0, 8, xh, z, oc),
            e_copy(r, 17, oh, zo, 0, 4, xh, z, oc),
            e_copy(r, 18, oh, zo, 4, 8, xh, z, oc),
        ]
        for r in range(2)
    ]

    def gate_rows(g, _):
        for a in range(4):
            s = g * 4 + a
            t = jnp.dot(swt[...], nbuf[pi, s], preferred_element_type=F32)
            gate[s] = jax.nn.sigmoid(t)
        return 0

    mine, other = pl.multiple_of(xl * TOK, TOK), pl.multiple_of(ol * TOK, TOK)

    def value_range(p, slot, c, lo, count):
        for a in range(count):
            s = lo + a
            v = jnp.dot(pwt[...], nbuf[p, s], preferred_element_type=F32).astype(BF16)
            vbuf[slot * 128 + s * 4 + c * 2] = v[:, 0:128]
            vbuf[slot * 128 + s * 4 + c * 2 + 1] = v[:, 128:256]

    def value_half(p, slot, c, g, _):
        value_range(p, slot, c, g * 16, 16)
        return 0

    def head_step(yy, slot, classes, lo, hi, with_total, g, _):
        n_rows = hi - lo
        v4 = vbuf.at[pl.ds(slot * 128 + lo * 4, n_rows * 4)]
        depth = len(classes) * TOK
        for a in range(H_UNROLL):
            h = g * H_UNROLL + a
            rows = pl.ds(pl.multiple_of(h * SPAN, SPAN), SPAN)
            weights = [ebuf[yy, h, pl.ds((mine, other)[c], TOK), :] for c in classes]
            weights = weights[0] if len(classes) == 1 else jnp.concatenate(weights, axis=0)
            v = v4[:, rows, :].reshape(n_rows, 4, SPAN, 128)
            v = jnp.concatenate(
                [v[:, 2 * c + t].reshape(n_rows * SPAN, 128) for c in classes for t in range(2)],
                axis=1,
            )
            if with_total:
                v = jnp.concatenate([v, jnp.ones((16, depth), BF16)], axis=0)
            part_sum = jnp.dot(v, weights, preferred_element_type=F32)
            acc[lo:hi, rows, :] += part_sum[:n_rows * SPAN].reshape(n_rows, SPAN, TOK)
            if with_total:
                tot[h] += part_sum[n_rows * SPAN:n_rows * SPAN + 8]
        return 0

    def values_of(p, slot, c):
        lax.fori_loop(0, ROWS // 16, functools.partial(value_half, p, slot, c), 0)

    def product_of(yy, slot, classes=(0, 1), lo=0, hi=ROWS, with_total=True):
        step = functools.partial(head_step, yy, slot, classes, lo, hi, with_total)
        lax.fori_loop(0, HEADS // H_UNROLL, step, 0)

    def hop(r, k, *then):
        e[r][k].wait_recv()
        for t in then:
            e[r][t].start()

    scores_of(0)
    n[18].start()
    scores_of(1)
    exps_of(0)
    for k in (2, 3, 1, 0):
        e[0][k].start()
    n[19].start()
    n[2].wait_recv()
    n[6].start()
    n[4].wait_recv()
    n[7].start()
    lax.fori_loop(0, ROWS // 4, gate_rows, 0)
    exps_of(1)
    for k in (2, 3, 1, 0):
        e[1][k].start()
    for k in (1, 8, 9):
        n[k].start()
    acc[...] = jnp.zeros_like(acc)
    tot[...] = jnp.zeros_like(tot)
    values_of(own, 0, 0)
    hop(0, 2, 7, 8)
    hop(0, 3, 9, 10)
    for k in (0, 18, 19):
        n[k].wait_recv()
    n[12].start()
    n[13].start()
    hop(0, 1, 4, 5, 6)
    hop(1, 2, 7, 8)
    hop(1, 3, 9, 10)
    n[3].wait_recv()
    n[14].start()
    n[5].wait_recv()
    n[15].start()
    values_of(pi_of(y3, xl), 2, 0)
    hop(1, 1, 4, 5, 6)
    n[6].wait_recv()
    n[10].start()
    n[7].wait_recv()
    n[11].start()
    hop(0, 7, 11)
    hop(0, 9, 12)
    values_of(pi_of(y1, xl), 1, 0)
    hop(1, 7, 11)
    hop(1, 9, 12)
    n[1].wait_recv()
    values_of(part, 0, 1)
    hop(0, 4, 13, 14)
    hop(0, 5, 15, 16)
    for r in range(2):
        for k in (0, 8, 10, 11, 12):
            e[r][k].wait_recv()
    product_of(y * (1 - swap) + y3 * swap, 2 * swap, (0,))
    hop(1, 4, 13, 14)
    hop(1, 5, 15, 16)
    n[12].wait_recv()
    n[16].start()
    n[13].wait_recv()
    n[17].start()
    n[8].wait_recv()
    values_of(pi_of(y3, ol), 2, 1)
    product_of(y * (1 - swap) + y3 * swap, 2 * swap, (1,))
    for r in range(2):
        hop(r, 13, 17)
        hop(r, 15, 18)
    for r in range(2):
        for k in (6, 14, 16, 17, 18):
            e[r][k].wait_recv()
    product_of(y3 * (1 - swap) + y * swap, 2 - 2 * swap)
    product_of(y1, 1, (0,))
    n[9].wait_recv()
    values_of(pi_of(y1, ol), 1, 1)
    product_of(y1, 1, (1,))
    n[14].wait_recv()
    n[15].wait_recv()
    values_of(b_o, 2 * swap, 0)
    product_of(yo, 2 * swap, (0,))

    def out_row(s):
        pieces = []
        for h in range(HEADS):
            rows = slice(h * SPAN, (h + 1) * SPAN)
            share = tot[h, 0:1, :]
            pieces.append((gate[s, rows, :] * (acc[s, rows, :] * share)).astype(BF16))
        mixed = jnp.concatenate(pieces, axis=0)
        out_ref[s] = jnp.dot(cw_ref[...], mixed, preferred_element_type=F32).astype(BF16)

    def last_rows(lo, hi, first):
        value_range(pi_of(yo, ol), 2 * swap, 1, lo, hi - lo)
        product_of(yo, 2 * swap, (1,), lo, hi, first)
        if first:
            for h in range(HEADS):
                tot[h] = 1.0 / tot[h]
        for s in range(lo, hi):
            out_row(s)

    n[16].wait_recv()
    n[17].wait_recv()
    last_rows(0, X_ROWS, True)
    n[10].wait_recv()
    n[11].wait_recv()
    last_rows(X_ROWS, ROWS, False)

    for c in n + e[0] + e[1]:
        c.wait_send()
    for r in range(2):
        for d in range(1, 16):
            m_copy(r, d).wait_send()


def body(duo, w, msa, gain, shift, pw, sw, cw):
    vm = pl.BlockSpec(memory_space=pltpu.VMEM)
    hbm = pl.BlockSpec(memory_space=pl.ANY)
    return pl.pallas_call(
        kernel,
        out_shape=pltpu.VMEM((ROWS, CH, TOK), BF16),
        in_specs=[hbm, vm, hbm] + [vm] * 5,
        out_specs=vm,
        scratch_shapes=[
            pltpu.VMEM((ROWS, CH, TOK), BF16),
            pltpu.VMEM((8, ROWS, CH, TOK), BF16),
            pltpu.VMEM((4, HEADS, 2 * TOK, TOK), BF16),
            pltpu.VMEM((256 * HEADS, 128), F32),
            pltpu.VMEM((2, 16, HEADS, 128), F32),
            pltpu.VMEM((ROWS, 256, TOK), F32),
            pltpu.VMEM((ROWS, 256, TOK), F32),
            pltpu.VMEM((3 * 128, 256, 128), BF16),
            pltpu.VMEM((HEADS, 8, TOK), F32),
            pltpu.VMEM((256, CH), BF16),
            pltpu.VMEM((256, CH), BF16),
            pltpu.VMEM((2, CH, TOK), F32),
            pltpu.SemaphoreType.DMA((2,)),
            pltpu.SemaphoreType.DMA((NPIECES,)),
            pltpu.SemaphoreType.DMA((20,)),
            pltpu.SemaphoreType.DMA((20,)),
            pltpu.SemaphoreType.DMA((2, 19)),
            pltpu.SemaphoreType.DMA((2, 19)),
            pltpu.SemaphoreType.DMA((2, 15)),
            pltpu.SemaphoreType.DMA((2, 15)),
        ],
        compiler_params=pltpu.CompilerParams(
            collective_id=0, has_side_effects=True, vmem_limit_bytes=65_000_000
        ),
        name="pair_average",
    )(duo.reshape(128, 256, 128), w.T, msa, gain.reshape(1, CH), shift.reshape(1, CH), pw, sw, cw.T)


def solution(mesh):
    placed = (P("pi", "pj", None), P(), P("pj", None, "pi"), P(), P(), P(), P(), P())
    return jax.shard_map(
        body, mesh=mesh, in_specs=placed, out_specs=P("pj", None, "pi"), check_vma=False
    )
```

```python
import functools

import jax
import jax.numpy as jnp
from jax import lax
from jax.experimental import pallas as pl
from jax.experimental.pallas import tpu as pltpu
from jax.sharding import PartitionSpec as P

EPS = 1e-05
F32 = jnp.float32
BF16 = jnp.bfloat16
MESH = pl.DeviceIdType.MESH
NT = (((1,), (1,)), ((), ()))

HEADS = 8
SPAN = 32
ROWS = 32
CH = 64
TOK = 256
X_ROWS = 21
NPIECES = 8
H_UNROLL = 8


def kernel(
    duo_hbm, wt_ref, msa_hbm, gain_ref, shift_ref, pw_ref, sw_ref, cw_ref,
    out_ref,
    msa, nbuf, ebuf, sc, mx, acc, gate, vbuf, tot, pwt, swt, gcol,
    msa_sem, duo_sem, n_send, n_recv, e_send, e_recv, m_send, m_recv,
):
    pi = lax.axis_index("pi")
    pj = lax.axis_index("pj")
    y, xl = lax.div(pi, 2), lax.rem(pi, 2)
    xh, zc = lax.div(pj, 8), lax.rem(pj, 8)
    z, core = lax.div(zc, 2), lax.rem(zc, 2)

    def pi_of(yy, ll):
        return yy * 2 + ll

    def pj_of(hh, zz, cc):
        return hh * 8 + zz * 2 + cc

    yp, ym, yo = lax.rem(y + 1, 4), lax.rem(y + 3, 4), lax.rem(y + 2, 4)
    zp, zm, zo = lax.rem(z + 1, 4), lax.rem(z + 3, 4), lax.rem(z + 2, 4)
    ol, oh = 1 - xl, 1 - xh
    y1, y3 = y + 1 - 2 * lax.rem(y, 2), 3 - y
    swap = lax.rem(lax.div(y, 2) + xh, 2)

    def msa_copy(k, lo, hi):
        rows = pl.ds(lo, hi - lo)
        return pltpu.make_async_copy(msa_hbm.at[rows], msa.at[rows], msa_sem.at[k])

    msa_in = [msa_copy(0, X_ROWS, ROWS), msa_copy(1, 0, X_ROWS)]
    for c in msa_in:
        c.start()

    step = 128 // NPIECES

    def duo_copy(k):
        rows = pl.ds(k * step, step)
        there = pl.ds(256 + k * step, step)
        return pltpu.make_async_copy(duo_hbm.at[rows], vbuf.at[there], duo_sem.at[k])

    barrier = pltpu.get_barrier_semaphore()
    for d in range(1, 16):
        pl.semaphore_signal(
            barrier, inc=1, device_id={"pi": pi, "pj": lax.rem(pj + d, 16)}, device_id_type=MESH
        )
    for other in (pi_of(yp, xl), pi_of(ym, xl), pi_of(y, ol)):
        pl.semaphore_signal(
            barrier, inc=1, device_id={"pi": other, "pj": pj}, device_id_type=MESH
        )

    for k in range(NPIECES):
        duo_copy(k).start()

    def column(ref):
        row = jnp.broadcast_to(ref[...], (CH, CH))
        r = lax.broadcasted_iota(jnp.int32, (CH, CH), 0)
        c = lax.broadcasted_iota(jnp.int32, (CH, CH), 1)
        col = jnp.sum(jnp.where(r == c, row, 0.0), axis=1, keepdims=True)
        return jnp.broadcast_to(col, (CH, TOK))

    gcol[0] = column(gain_ref)
    gcol[1] = column(shift_ref)

    def norm_range(lo, hi):
        for s in range(lo, hi):
            v = msa[s].astype(F32)
            mean = jnp.mean(v, axis=0, keepdims=True)
            v = v - mean
            var = jnp.mean(v * v, axis=0, keepdims=True)
            v = v * lax.rsqrt(var + EPS)
            nbuf[pi, s] = (v * gcol[0] + gcol[1]).astype(BF16)

    xa, xb = X_ROWS // 2, X_ROWS
    ya, yb = X_ROWS + (ROWS - X_ROWS) // 2, ROWS

    def n_copy(k, block, lo, hi, to_y, to_l):
        view = nbuf.at[block, pl.ds(lo, hi - lo)]
        return pltpu.make_async_remote_copy(
            src_ref=view, dst_ref=view, send_sem=n_send.at[k], recv_sem=n_recv.at[k],
            device_id={"pi": pi_of(to_y, to_l), "pj": pj}, device_id_type=MESH,
        )

    own, part = pi, pi_of(y, ol)
    b_m, b_p, b_o = pi_of(ym, xl), pi_of(yp, xl), pi_of(yo, xl)
    q_m, q_p = pi_of(ym, ol), pi_of(yp, ol)
    n = [
        n_copy(0, own, 0, 6, y, ol),
        n_copy(1, own, xb, yb, y, ol),
        n_copy(2, own, xb, yb, yp, xl),
        n_copy(3, own, 0, xb, yp, xl),
        n_copy(4, own, xb, yb, ym, xl),
        n_copy(5, own, 0, xb, ym, xl),
        n_copy(6, b_m, xb, ya, yp, xl),
        n_copy(7, b_p, ya, yb, ym, xl),
        n_copy(8, pi_of(y3, xl), xb, yb, y, ol),
        n_copy(9, pi_of(y1, xl), xb, yb, y, ol),
        n_copy(10, b_o, xb, ya, y, ol),
        n_copy(11, b_o, ya, yb, y, ol),
        n_copy(12, part, 0, xb, yp, xl),
        n_copy(13, part, 0, xb, ym, xl),
        n_copy(14, b_m, 0, xa, yp, xl),
        n_copy(15, b_p, xa, xb, ym, xl),
        n_copy(16, q_m, 0, xa, yp, xl),
        n_copy(17, q_p, xa, xb, ym, xl),
        n_copy(18, own, 6, 14, y, ol),
        n_copy(19, own, 14, xb, y, ol),
    ]
    msa_in[0].wait()
    norm_range(X_ROWS, ROWS)
    pl.semaphore_wait(barrier, 18)
    for k in (2, 4):
        n[k].start()
    msa_in[1].wait()
    norm_range(0, 6)
    n[0].start()
    norm_range(6, X_ROWS)
    for k in (3, 5):
        n[k].start()

    pwt[...] = pw_ref[...].astype(F32).T.astype(BF16)
    swt[...] = sw_ref[...].astype(F32).T.astype(BF16)

    w = wt_ref[...]
    w = w - jnp.mean(w, axis=1, keepdims=True)
    w_sum = jnp.sum(w, axis=1, keepdims=True)
    w_hi = w.astype(BF16)
    w_rest = w - w_hi.astype(F32)
    w_mid = w_rest.astype(BF16)
    w_lo = (w_rest - w_mid.astype(F32)).astype(BF16)
    ones8 = jnp.ones((8, 128), F32)
    stack = jnp.concatenate(
        [w_hi.astype(F32), w_mid.astype(F32), w_lo.astype(F32), ones8], axis=0
    ).astype(BF16)
    ones = jnp.ones((16, 128), BF16)
    group = 16

    def score_group(g, _):
        x = vbuf[pl.ds(256 + g * (group // 2), group // 2)].reshape(group * 128, 128)
        xf = x.astype(F32)
        sq = xf * xf
        sq_hi = sq.astype(BF16)
        sq_lo = (sq - sq_hi.astype(F32)).astype(BF16)
        r = lax.dot_general(stack, x, NT, preferred_element_type=F32)
        t_hi = lax.dot_general(ones, sq_hi, NT, preferred_element_type=F32)[0:8]
        t_lo = lax.dot_general(ones, sq_lo, NT, preferred_element_type=F32)[0:8]
        mean = r[24:32] * (1.0 / 128)
        m_hi = mean.astype(BF16).astype(F32)
        m_lo = mean - m_hi
        var = t_hi * (1.0 / 128) - m_hi * m_hi
        var = var - 2.0 * m_hi * m_lo
        var = (var - m_lo * m_lo) + t_lo * (1.0 / 128)
        var = jnp.maximum(var, 0.0)
        dots = (r[16:24] + r[8:16]) + r[0:8]
        s = (dots - mean * w_sum) * lax.rsqrt(var + EPS)
        for a in range(group):
            rows = pl.ds(pl.multiple_of((g * group + a) * 8, 8), 8)
            sc[rows, :] = s[:, a * 128:(a + 1) * 128]
        return 0

    per = 2 * step // group

    def score_piece(k, _):
        duo_copy(k).wait()
        lax.fori_loop(k * per, (k + 1) * per, score_group, 0)
        return 0

    def m_copy(r, d):
        view = mx.at[r, pj]
        return pltpu.make_async_remote_copy(
            src_ref=view, dst_ref=view, send_sem=m_send.at[r, d - 1],
            recv_sem=m_recv.at[r, d - 1],
            device_id={"pi": pi, "pj": lax.rem(pj + d, 16)}, device_id_type=MESH,
        )

    def scores_of(r):
        lax.fori_loop(r * NPIECES // 2, (r + 1) * NPIECES // 2, score_piece, 0)
        for h in range(HEADS):
            t = sc[pl.ds(r * 1024 + h, 128, stride=8), :].T
            acc[8 + h, 0:128, r * 128:(r + 1) * 128] = t
            mx[r, pj, pl.ds(h, 1), :] = jnp.max(t, axis=0, keepdims=True)
        for d in range(1, 16):
            m_copy(r, d).start()

    def columns(zz, cc):
        return pl.ds(pl.multiple_of(lax.rem(zz, 2) * 256 + cc * 128, 128), 128)

    def pair_of(hh, zz):
        return hh * 2 + lax.div(zz, 2)

    def exps_of(r):
        for d in range(1, 16):
            m_copy(r, d).wait_recv()
        peak = mx[r, 0]
        for d in range(1, 16):
            peak = jnp.maximum(peak, mx[r, d])
        lanes = slice(r * 128, (r + 1) * 128)
        for h in range(HEADS):
            t = jnp.exp(acc[8 + h, 0:128, lanes] - peak[h:h + 1])
            ebuf[pair_of(xh, z), h, columns(z, core), lanes] = t.astype(BF16)

    def e_copy(r, k, hh, zz, h0, h1, to_h, to_z, to_c):
        view = ebuf.at[
            pair_of(hh, zz), pl.ds(h0, h1 - h0), columns(zz, core), pl.ds(r * 128, 128)
        ]
        return pltpu.make_async_remote_copy(
            src_ref=view, dst_ref=view, send_sem=e_send.at[r, k], recv_sem=e_recv.at[r, k],
            device_id={"pi": pi, "pj": pj_of(to_h, to_z, to_c)}, device_id_type=MESH,
        )

    oc = 1 - core
    e = [
        [
            e_copy(r, 0, xh, z, 0, 8, xh, z, oc),
            e_copy(r, 1, xh, z, 0, 8, oh, z, core),
            e_copy(r, 2, xh, z, 0, 8, xh, zp, core),
            e_copy(r, 3, xh, z, 0, 8, xh, zm, core),
            e_copy(r, 4, oh, z, 0, 8, xh, zp, core),
            e_copy(r, 5, oh, z, 0, 8, xh, zm, core),
            e_copy(r, 6, oh, z, 0, 8, xh, z, oc),
            e_copy(r, 7, xh, zm, 0, 4, xh, zp, core),
            e_copy(r, 8, xh, zm, 0, 8, xh, z, oc),
            e_copy(r, 9, xh, zp, 4, 8, xh, zm, core),
            e_copy(r, 10, xh, zp, 0, 8, xh, z, oc),
            e_copy(r, 11, xh, zo, 0, 4, xh, z, oc),
            e_copy(r, 12, xh, zo, 4, 8, xh, z, oc),
            e_copy(r, 13, oh, zm, 0, 4, xh, zp, core),
            e_copy(r, 14, oh, zm, 0, 8, xh, z, oc),
            e_copy(r, 15, oh, zp, 4, 8, xh, zm, core),
            e_copy(r, 16, oh, zp, 0, 8, xh, z, oc),
            e_copy(r, 17, oh, zo, 0, 4, xh, z, oc),
            e_copy(r, 18, oh, zo, 4, 8, xh, z, oc),
        ]
        for r in range(2)
    ]

    def gate_rows(g, _):
        for a in range(4):
            s = g * 4 + a
            t = jnp.dot(swt[...], nbuf[pi, s], preferred_element_type=F32)
            gate[s] = jax.nn.sigmoid(t)
        return 0

    mine, other = pl.multiple_of(xl * TOK, TOK), pl.multiple_of(ol * TOK, TOK)

    def value_range(p, slot, c, lo, count):
        for a in range(count):
            s = lo + a
            v = jnp.dot(pwt[...], nbuf[p, s], preferred_element_type=F32).astype(BF16)
            vbuf[slot * 128 + s * 4 + c * 2] = v[:, 0:128]
            vbuf[slot * 128 + s * 4 + c * 2 + 1] = v[:, 128:256]

    def head_step(yy, slot, classes, lo, hi, with_total, g, _):
        n_rows = hi - lo
        v4 = vbuf.at[pl.ds(slot * 128 + lo * 4, n_rows * 4)]
        depth = len(classes) * TOK
        for a in range(H_UNROLL):
            h = g * H_UNROLL + a
            rows = pl.ds(pl.multiple_of(h * SPAN, SPAN), SPAN)
            weights = [ebuf[yy, h, pl.ds((mine, other)[c], TOK), :] for c in classes]
            weights = weights[0] if len(classes) == 1 else jnp.concatenate(weights, axis=0)
            v = v4[:, rows, :].reshape(n_rows, 4, SPAN, 128)
            v = jnp.concatenate(
                [v[:, 2 * c + t].reshape(n_rows * SPAN, 128) for c in classes for t in range(2)],
                axis=1,
            )
            if with_total:
                v = jnp.concatenate([v, jnp.ones((16, depth), BF16)], axis=0)
            part_sum = jnp.dot(v, weights, preferred_element_type=F32)
            acc[lo:hi, rows, :] += part_sum[:n_rows * SPAN].reshape(n_rows, SPAN, TOK)
            if with_total:
                tot[h] += part_sum[n_rows * SPAN:n_rows * SPAN + 8]
        return 0

    def values_of(p, slot, c):
        value_range(p, slot, c, 0, ROWS)

    def product_of(yy, slot, classes=(0, 1), lo=0, hi=ROWS, with_total=True):
        step = functools.partial(head_step, yy, slot, classes, lo, hi, with_total)
        lax.fori_loop(0, HEADS // H_UNROLL, step, 0)

    def hop(r, k, *then):
        e[r][k].wait_recv()
        for t in then:
            e[r][t].start()

    scores_of(0)
    n[18].start()
    scores_of(1)
    exps_of(0)
    for k in (2, 3, 1, 0):
        e[0][k].start()
    n[19].start()
    n[2].wait_recv()
    n[6].start()
    n[4].wait_recv()
    n[7].start()
    lax.fori_loop(0, ROWS // 4, gate_rows, 0)
    exps_of(1)
    for k in (2, 3, 1, 0):
        e[1][k].start()
    for k in (1, 8, 9):
        n[k].start()
    acc[...] = jnp.zeros_like(acc)
    tot[...] = jnp.zeros_like(tot)
    values_of(own, 0, 0)
    hop(0, 2, 7, 8)
    hop(0, 3, 9, 10)
    for k in (0, 18, 19):
        n[k].wait_recv()
    n[12].start()
    n[13].start()
    hop(0, 1, 4, 5, 6)
    hop(1, 2, 7, 8)
    hop(1, 3, 9, 10)
    n[3].wait_recv()
    n[14].start()
    n[5].wait_recv()
    n[15].start()
    values_of(pi_of(y3, xl), 2, 0)
    hop(1, 1, 4, 5, 6)
    n[6].wait_recv()
    n[10].start()
    n[7].wait_recv()
    n[11].start()
    hop(0, 7, 11)
    hop(0, 9, 12)
    values_of(pi_of(y1, xl), 1, 0)
    hop(1, 7, 11)
    hop(1, 9, 12)
    n[1].wait_recv()
    values_of(part, 0, 1)
    hop(0, 4, 13, 14)
    hop(0, 5, 15, 16)
    for r in range(2):
        for k in (0, 8, 10, 11, 12):
            e[r][k].wait_recv()
    product_of(y * (1 - swap) + y3 * swap, 2 * swap, (0,))
    hop(1, 4, 13, 14)
    hop(1, 5, 15, 16)
    n[12].wait_recv()
    n[16].start()
    n[13].wait_recv()
    n[17].start()
    n[8].wait_recv()
    values_of(pi_of(y3, ol), 2, 1)
    product_of(y * (1 - swap) + y3 * swap, 2 * swap, (1,))
    for r in range(2):
        hop(r, 13, 17)
        hop(r, 15, 18)
    for r in range(2):
        for k in (6, 14, 16, 17, 18):
            e[r][k].wait_recv()
    product_of(y3 * (1 - swap) + y * swap, 2 - 2 * swap)
    product_of(y1, 1, (0,))
    n[9].wait_recv()
    values_of(pi_of(y1, ol), 1, 1)
    product_of(y1, 1, (1,))
    n[14].wait_recv()
    n[15].wait_recv()
    values_of(b_o, 2 * swap, 0)
    product_of(yo, 2 * swap, (0,))

    def out_row(s):
        pieces = []
        for h in range(HEADS):
            rows = slice(h * SPAN, (h + 1) * SPAN)
            share = tot[h, 0:1, :]
            pieces.append((gate[s, rows, :] * (acc[s, rows, :] * share)).astype(BF16))
        mixed = jnp.concatenate(pieces, axis=0)
        out_ref[s] = jnp.dot(cw_ref[...], mixed, preferred_element_type=F32).astype(BF16)

    def last_rows(lo, hi, first):
        value_range(pi_of(yo, ol), 2 * swap, 1, lo, hi - lo)
        product_of(yo, 2 * swap, (1,), lo, hi, first)
        if first:
            for h in range(HEADS):
                tot[h] = 1.0 / tot[h]
        for s in range(lo, hi):
            out_row(s)

    n[16].wait_recv()
    n[17].wait_recv()
    last_rows(0, X_ROWS, True)
    n[10].wait_recv()
    n[11].wait_recv()
    last_rows(X_ROWS, ROWS, False)

    for c in n + e[0] + e[1]:
        c.wait_send()
    for r in range(2):
        for d in range(1, 16):
            m_copy(r, d).wait_send()


def body(duo, w, msa, gain, shift, pw, sw, cw):
    vm = pl.BlockSpec(memory_space=pltpu.VMEM)
    hbm = pl.BlockSpec(memory_space=pl.ANY)
    return pl.pallas_call(
        kernel,
        out_shape=pltpu.VMEM((ROWS, CH, TOK), BF16),
        in_specs=[hbm, vm, hbm] + [vm] * 5,
        out_specs=vm,
        scratch_shapes=[
            pltpu.VMEM((ROWS, CH, TOK), BF16),
            pltpu.VMEM((8, ROWS, CH, TOK), BF16),
            pltpu.VMEM((4, HEADS, 2 * TOK, TOK), BF16),
            pltpu.VMEM((256 * HEADS, 128), F32),
            pltpu.VMEM((2, 16, HEADS, 128), F32),
            pltpu.VMEM((ROWS, 256, TOK), F32),
            pltpu.VMEM((ROWS, 256, TOK), F32),
            pltpu.VMEM((3 * 128, 256, 128), BF16),
            pltpu.VMEM((HEADS, 8, TOK), F32),
            pltpu.VMEM((256, CH), BF16),
            pltpu.VMEM((256, CH), BF16),
            pltpu.VMEM((2, CH, TOK), F32),
            pltpu.SemaphoreType.DMA((2,)),
            pltpu.SemaphoreType.DMA((NPIECES,)),
            pltpu.SemaphoreType.DMA((20,)),
            pltpu.SemaphoreType.DMA((20,)),
            pltpu.SemaphoreType.DMA((2, 19)),
            pltpu.SemaphoreType.DMA((2, 19)),
            pltpu.SemaphoreType.DMA((2, 15)),
            pltpu.SemaphoreType.DMA((2, 15)),
        ],
        compiler_params=pltpu.CompilerParams(
            collective_id=0, has_side_effects=True, vmem_limit_bytes=65_000_000
        ),
        name="pair_average",
    )(duo.reshape(128, 256, 128), w.T, msa, gain.reshape(1, CH), shift.reshape(1, CH), pw, sw, cw.T)


def solution(mesh):
    placed = (P("pi", "pj", None), P(), P("pj", None, "pi"), P(), P(), P(), P(), P())
    return jax.shard_map(
        body, mesh=mesh, in_specs=placed, out_specs=P("pj", None, "pi"), check_vma=False
    )
```
